32 devices in a mesh: batch: 1 (over z), dap: 32 (over y, x, core).
Axes of the slice: x: 4, y: 4, z: 1, core: 2. Of those that a mesh axis runs over, the one named last changes fastest.
The devices are a block of a 4x4x8 slice.
Arguments:
- pair_act: bfloat16 [512, 512, 128], P(('batch', 'dap'))
- pair_mask: int32 [512, 512], P(('batch', 'dap'))
- msa_act: bfloat16 [512, 512, 256], P(None, ('batch', 'dap'))
- opm_norm: bfloat16 [2, 2, 256], replicated
- opm_w_in: bfloat16 [2, 256, 2, 32], replicated
- opm_b_in: bfloat16 [2, 2, 32], replicated
- opm_w_out: bfloat16 [2, 1024, 128], replicated
- opm_b_out: bfloat16 [2, 128], replicated
- tri_norm_in: bfloat16 [2, 2, 128], replicated
- tri_w_ab: bfloat16 [2, 128, 4, 128], replicated
- tri_b_ab: bfloat16 [2, 4, 128], replicated
- tri_w_gate: bfloat16 [2, 128, 128], replicated
- tri_b_gate: bfloat16 [2, 128], replicated
- tri_norm_out: bfloat16 [2, 2, 128], replicated
- tri_w_out: bfloat16 [2, 128, 128], replicated
- tri_b_out: bfloat16 [2, 128], replicated
Outputs:
- output: bfloat16 [512, 512, 128], P(('batch', 'dap'))
All inputs are finite; a program needn't handle non-finite values.
Results may differ from the reference program's by a relative error of at most 0.0110511.
Values are sent between devices in bfloat16 or wider.
A program may use at most 768 MiB of HBM per device.

```python
import jax
import jax.numpy as jnp
from jax import lax

RESIDUES = 512
MSA_ROWS = 512
PAIR_DIM = 128
TRI_DIM = 128
MSA_DIM = 256
OPM_DIM = 32
LAYERS = 2
ROW_BLOCK = 8

LN_EPS = 1e-5


def normal_draw(base_key, arr_shape, draw_scale):
    return (draw_scale * jax.random.normal(base_key, arr_shape, jnp.float32)).astype(jnp.bfloat16)


def norm_draw(base_key, arr_shape):
    noise_val = 0.3 * jax.random.normal(base_key, arr_shape, jnp.float32)
    return (noise_val + jnp.array([1.0, 0.0], jnp.float32)[None, :, None]).astype(jnp.bfloat16)


def setup_inputs(seed: int = 0, part: int = 0) -> dict:
    part_keys = jax.random.split(jax.random.fold_in(jax.random.key(seed), part), 6)
    weight_keys = jax.random.split(jax.random.key(seed + 1), 13)
    row_part = jax.random.normal(part_keys[0], (RESIDUES, 1, PAIR_DIM), jnp.float32)
    col_part = jax.random.normal(part_keys[1], (1, RESIDUES, PAIR_DIM), jnp.float32)
    pair_noise = jax.random.normal(part_keys[2], (RESIDUES, RESIDUES, PAIR_DIM), jnp.float32)
    pair_act = (0.6 * row_part + 0.6 * col_part + 0.5 * pair_noise).astype(jnp.bfloat16)
    profile = jax.random.normal(part_keys[3], (1, RESIDUES, MSA_DIM), jnp.float32)
    msa_noise = jax.random.normal(part_keys[4], (MSA_ROWS, RESIDUES, MSA_DIM), jnp.float32)
    msa_act = (0.8 * profile + 0.6 * msa_noise).astype(jnp.bfloat16)
    valid_len = RESIDUES // 2 + jax.random.randint(part_keys[5], (), 0, RESIDUES // 2 + 1)
    seq_valid = (jnp.arange(RESIDUES) < valid_len).astype(jnp.int32)
    pair_mask = seq_valid[:, None] * seq_valid[None, :]
    return {
        'pair_act': pair_act,
        'pair_mask': pair_mask,
        'msa_act': msa_act,
        'opm_norm': norm_draw(weight_keys[0], (LAYERS, 2, MSA_DIM)),
        'opm_w_in': normal_draw(weight_keys[1], (LAYERS, MSA_DIM, 2, OPM_DIM), MSA_DIM ** -0.5),
        'opm_b_in': normal_draw(weight_keys[2], (LAYERS, 2, OPM_DIM), 0.5),
        'opm_w_out': normal_draw(weight_keys[3], (LAYERS, OPM_DIM * OPM_DIM, PAIR_DIM), (OPM_DIM * OPM_DIM) ** -0.5),
        'opm_b_out': normal_draw(weight_keys[4], (LAYERS, PAIR_DIM), 0.5),
        'tri_norm_in': norm_draw(weight_keys[5], (LAYERS, 2, PAIR_DIM)),
        'tri_w_ab': normal_draw(weight_keys[6], (LAYERS, PAIR_DIM, 4, TRI_DIM), PAIR_DIM ** -0.5),
        'tri_b_ab': normal_draw(weight_keys[7], (LAYERS, 4, TRI_DIM), 0.3),
        'tri_w_gate': normal_draw(weight_keys[8], (LAYERS, PAIR_DIM, PAIR_DIM), PAIR_DIM ** -0.5),
        'tri_b_gate': normal_draw(weight_keys[9], (LAYERS, PAIR_DIM), 0.5),
        'tri_norm_out': norm_draw(weight_keys[10], (LAYERS, 2, TRI_DIM)),
        'tri_w_out': normal_draw(weight_keys[11], (LAYERS, TRI_DIM, PAIR_DIM), TRI_DIM ** -0.5),
        'tri_b_out': normal_draw(weight_keys[12], (LAYERS, PAIR_DIM), 0.5),
    }


def layer_norm(values, norm_gains):
    x_f32 = values.astype(jnp.float32)
    mean_val = jnp.mean(x_f32, axis=-1, keepdims=True)
    centered = x_f32 - mean_val
    var_val = jnp.mean(centered * centered, axis=-1, keepdims=True)
    scaled = centered * lax.rsqrt(var_val + LN_EPS)
    return (scaled * norm_gains[0].astype(jnp.float32) + norm_gains[1].astype(jnp.float32)).astype(jnp.bfloat16)


def outer_mean_update(pair_act, msa_act, norm_w, w_in, b_in, w_out, b_out):
    msa_norm = layer_norm(msa_act, norm_w).astype(jnp.float32)
    w_in_f = w_in.astype(jnp.float32)
    b_in_f = b_in.astype(jnp.float32)
    left_proj = (jnp.einsum('snm,mc->snc', msa_norm, w_in_f[:, 0, :]) + b_in_f[0]).astype(jnp.bfloat16).astype(jnp.float32)
    right_proj = (jnp.einsum('snm,mc->snc', msa_norm, w_in_f[:, 1, :]) + b_in_f[1]).astype(jnp.bfloat16).astype(jnp.float32)
    w_out_f = w_out.astype(jnp.float32).reshape(OPM_DIM, OPM_DIM, PAIR_DIM)
    b_out_f = b_out.astype(jnp.float32)
    num_blocks = RESIDUES // ROW_BLOCK
    left_blocks = jnp.moveaxis(left_proj.reshape(MSA_ROWS, num_blocks, ROW_BLOCK, OPM_DIM), 1, 0)
    pair_blocks = pair_act.reshape(num_blocks, ROW_BLOCK, RESIDUES, PAIR_DIM)

    def block_update(block_args):
        left_blk, pair_blk = block_args
        outer_prod = jnp.einsum('sic,sjd->ijcd', left_blk, right_proj) / MSA_ROWS
        outer_prod = outer_prod.astype(jnp.bfloat16).astype(jnp.float32)
        pair_upd = (jnp.einsum('ijcd,cdz->ijz', outer_prod, w_out_f) + b_out_f).astype(jnp.bfloat16)
        return (pair_blk.astype(jnp.float32) + pair_upd.astype(jnp.float32)).astype(jnp.bfloat16)

    return lax.map(block_update, (left_blocks, pair_blocks)).reshape(RESIDUES, RESIDUES, PAIR_DIM)


def triangle_update(pair_act, mask_f, norm_in, w_ab, b_ab, w_gate, b_gate, norm_out, w_out, b_out):
    num_blocks = RESIDUES // ROW_BLOCK
    pair_blocks = pair_act.reshape(num_blocks, ROW_BLOCK, RESIDUES, PAIR_DIM)
    mask_blocks = mask_f.reshape(num_blocks, ROW_BLOCK, RESIDUES)
    w_ab_f = w_ab.astype(jnp.float32)
    b_ab_f = b_ab.astype(jnp.float32)
    w_gate_f = w_gate.astype(jnp.float32)
    b_gate_f = b_gate.astype(jnp.float32)
    w_out_f = w_out.astype(jnp.float32)
    b_out_f = b_out.astype(jnp.float32)

    def project_block(block_args):
        pair_blk, mask_blk = block_args
        normed = layer_norm(pair_blk, norm_in).astype(jnp.float32)
        projected = jnp.einsum('ikz,zqc->qikc', normed, w_ab_f) + b_ab_f[:, None, None, :]
        mask_col = mask_blk[:, :, None]
        left_val = (mask_col * jax.nn.sigmoid(projected[1]) * projected[0]).astype(jnp.bfloat16)
        right_val = (mask_col * jax.nn.sigmoid(projected[3]) * projected[2]).astype(jnp.bfloat16)
        return left_val, right_val

    left_all, right_all = lax.map(project_block, (pair_blocks, mask_blocks))
    right_f = right_all.reshape(RESIDUES, RESIDUES, TRI_DIM).astype(jnp.float32)

    def update_block(block_args):
        pair_blk, left_blk = block_args
        normed = layer_norm(pair_blk, norm_in).astype(jnp.float32)
        gate_val = jax.nn.sigmoid(jnp.einsum('ikz,zy->iky', normed, w_gate_f) + b_gate_f)
        tri_prod = jnp.einsum('ikc,jkc->ijc', left_blk.astype(jnp.float32), right_f)
        prod_norm = layer_norm(tri_prod, norm_out).astype(jnp.float32)
        pair_upd = (jnp.einsum('ijc,cz->ijz', prod_norm, w_out_f) + b_out_f).astype(jnp.bfloat16)
        return (pair_blk.astype(jnp.float32) + gate_val * pair_upd.astype(jnp.float32)).astype(jnp.bfloat16)

    return lax.map(update_block, (pair_blocks, left_all)).reshape(RESIDUES, RESIDUES, PAIR_DIM)


def reference(pair_act, pair_mask, msa_act, opm_norm, opm_w_in, opm_b_in, opm_w_out, opm_b_out, tri_norm_in, tri_w_ab, tri_b_ab, tri_w_gate, tri_b_gate, tri_norm_out, tri_w_out, tri_b_out):
    mask_f = pair_mask.astype(jnp.float32)
    for layer_idx in range(LAYERS):
        pair_act = outer_mean_update(pair_act, msa_act, opm_norm[layer_idx], opm_w_in[layer_idx], opm_b_in[layer_idx], opm_w_out[layer_idx], opm_b_out[layer_idx])
        pair_act = triangle_update(pair_act, mask_f, tri_norm_in[layer_idx], tri_w_ab[layer_idx], tri_b_ab[layer_idx], tri_w_gate[layer_idx], tri_b_gate[layer_idx], tri_norm_out[layer_idx], tri_w_out[layer_idx], tri_b_out[layer_idx])
    return pair_act
```

```python
import math
import jax
import jax.numpy as jnp
from jax import lax
from jax.sharding import PartitionSpec as P

LN_EPS = 1e-5
ROW_BLOCK = 8


def layer_norm(values, gain_scale, offset, norm_axis):
    x_f32 = values.astype(jnp.float32)
    mean_val = jnp.mean(x_f32, axis=norm_axis, keepdims=True)
    centered = x_f32 - mean_val
    var_val = jnp.mean(centered * centered, axis=norm_axis, keepdims=True)
    return (centered * lax.rsqrt(var_val + LN_EPS) * gain_scale + offset).astype(jnp.bfloat16)


def value_a15(value_a7, norm_w, w_in, b_in):
    normed = layer_norm(value_a7, norm_w[0].astype(jnp.float32), norm_w[1].astype(jnp.float32), -1)
    in_bias = b_in.astype(jnp.float32)
    left_proj = (jnp.einsum('sim,mc->sic', normed, w_in[:, 0, :], preferred_element_type=jnp.float32) + in_bias[0]).astype(jnp.bfloat16)
    right_proj = (jnp.einsum('sim,mc->sic', normed, w_in[:, 1, :], preferred_element_type=jnp.float32) + in_bias[1]).astype(jnp.bfloat16)
    return left_proj, right_proj


def outer_mean_rows(pair_act, left_proj, right_full, w_out, b_out):
    row_count, col_count, pair_dim = pair_act.shape
    value_a9 = left_proj.shape[0]
    opm_dim = left_proj.shape[2]
    row_blk = math.gcd(row_count, ROW_BLOCK)
    num_blocks = row_count // row_blk
    left_blocks = jnp.moveaxis(left_proj.reshape(value_a9, num_blocks, row_blk, opm_dim), 1, 0)
    pair_blocks = pair_act.reshape(num_blocks, row_blk, col_count, pair_dim)
    w_out_r = w_out.reshape(opm_dim, opm_dim, pair_dim)
    out_bias = b_out.astype(jnp.float32)

    def block_update(block_args):
        left_blk, pair_blk = block_args
        outer_prod = jnp.einsum('sic,sjd->icjd', left_blk, right_full, preferred_element_type=jnp.float32)
        outer_prod = (outer_prod / value_a9).astype(jnp.bfloat16)
        pair_upd = (jnp.einsum('icjd,cdz->ijz', outer_prod, w_out_r, preferred_element_type=jnp.float32) + out_bias).astype(jnp.bfloat16)
        return (pair_blk.astype(jnp.float32) + pair_upd.astype(jnp.float32)).astype(jnp.bfloat16)

    return lax.map(block_update, (left_blocks, pair_blocks)).reshape(row_count, col_count, pair_dim)


def gated_projection(normed, mask_f, w_pair, b_pair):
    projected = jnp.einsum('zqc,ikz->qcik', w_pair, normed, preferred_element_type=jnp.float32)
    projected = projected + b_pair.astype(jnp.float32)[:, :, None, None]
    return (mask_f[None] * jax.nn.sigmoid(projected[1]) * projected[0]).astype(jnp.bfloat16)


def triangle_finish(pair_act, normed, tri_prod, w_gate, b_gate, norm_out, w_out, b_out):
    gate_val = jax.nn.sigmoid(jnp.einsum('ikz,zy->iky', normed, w_gate, preferred_element_type=jnp.float32) + b_gate.astype(jnp.float32))
    out_gains = norm_out.astype(jnp.float32)[:, :, None, None]
    prod_norm = layer_norm(tri_prod, out_gains[0], out_gains[1], 0)
    pair_upd = (jnp.einsum('cij,cz->ijz', prod_norm, w_out, preferred_element_type=jnp.float32) + b_out.astype(jnp.float32)).astype(jnp.bfloat16)
    return (pair_act.astype(jnp.float32) + gate_val * pair_upd.astype(jnp.float32)).astype(jnp.bfloat16)


def solution(mesh):
    pair_spec = P(('batch', 'dap'), None, None)
    mask_spec = P(('batch', 'dap'), None)
    array_b8 = P(None, ('batch', 'dap'), None)

    def device_fn(pair_act, pair_mask, value_a7, opm_norm, opm_w_in, opm_b_in, opm_w_out, opm_b_out, tri_norm_in, tri_w_ab, tri_b_ab, tri_w_gate, tri_b_gate, tri_norm_out, tri_w_out, tri_b_out):
        mask_f = pair_mask.astype(jnp.float32)
        for layer_idx in range(opm_norm.shape[0]):
            value_a8, array_b9 = value_a15(value_a7, opm_norm[layer_idx], opm_w_in[layer_idx], opm_b_in[layer_idx])
            value_a14 = lax.all_gather(array_b9, 'dap', axis=1, tiled=True)
            pair_act = outer_mean_rows(pair_act, value_a8, value_a14, opm_w_out[layer_idx], opm_b_out[layer_idx])
            norm_in = tri_norm_in[layer_idx].astype(jnp.float32)
            normed = layer_norm(pair_act, norm_in[0], norm_in[1], -1)
            w_ab = tri_w_ab[layer_idx]
            b_ab = tri_b_ab[layer_idx]
            right_tri = gated_projection(normed, mask_f, w_ab[:, 2:4], b_ab[2:4])
            right_ch = lax.all_to_all(right_tri, 'dap', 0, 1, tiled=True)
            left_tri = gated_projection(normed, mask_f, w_ab[:, 0:2], b_ab[0:2])
            left_ch = lax.all_to_all(left_tri, 'dap', 0, 1, tiled=True)
            tri_ch = jnp.einsum('cik,cjk->cij', left_ch, right_ch, preferred_element_type=jnp.float32)
            tri_prod = lax.all_to_all(tri_ch, 'dap', 1, 0, tiled=True)
            pair_act = triangle_finish(pair_act, normed, tri_prod, tri_w_gate[layer_idx], tri_b_gate[layer_idx], tri_norm_out[layer_idx], tri_w_out[layer_idx], tri_b_out[layer_idx])
        return pair_act

    return jax.shard_map(device_fn, mesh=mesh, in_specs=(pair_spec, mask_spec, array_b8) + (P(),) * 13, out_specs=pair_spec, check_vma=False)
```

```python
import functools
import math
import jax
import jax.numpy as jnp
from jax import lax
from jax.experimental import pallas as pl
from jax.experimental.pallas import tpu as pltpu
from jax.sharding import PartitionSpec as P

LN_EPS = 1e-5
LANES = 128
AG_CHUNKS = 1
F32 = jnp.float32
BF16 = jnp.bfloat16


def dot_nn(a, b):
    return lax.dot_general(a, b, (((1,), (0,)), ((), ())), preferred_element_type=F32)


def dot_nt(a, b):
    return lax.dot_general(a, b, (((1,), (1,)), ((), ())), preferred_element_type=F32)


I_STRIDE = 24
S_GROUP = 16


def msa_kernel(m_ref, norm_ref, w_ref, bias_ref, a_ref, b_ref, y_ref, t_ref):
    s_blk, n_i, _ = m_ref.shape
    layers, n_c = a_ref.shape[0], b_ref.shape[1]
    group = S_GROUP

    def rows(g, carry):
        base = pl.multiple_of(g * group, group)
        x = m_ref[pl.ds(base, group)].astype(F32).reshape(group * n_i, -1)
        mean_val = jnp.mean(x, axis=-1, keepdims=True)
        centered = x - mean_val
        var_val = jnp.mean(centered * centered, axis=-1, keepdims=True)
        scaled = centered * lax.rsqrt(var_val + LN_EPS)
        normed = jnp.concatenate([(scaled * norm_ref[l, 0:1] + norm_ref[l, 1:2]).astype(BF16) for l in range(layers)], axis=1)
        proj = dot_nn(normed, w_ref[...]) + bias_ref[...]
        for s in range(group):
            y_ref[pl.ds(pl.multiple_of((base + s) * I_STRIDE, 8), n_i), :] = proj[s * n_i:(s + 1) * n_i]
        return carry
    lax.fori_loop(0, s_blk // group, rows, 0)

    def columns(i, carry):
        flip = y_ref[pl.ds(i, s_blk, stride=I_STRIDE), :].T
        for l in range(layers):
            top = 2 * l * n_c
            a_ref[l, pl.ds(pl.multiple_of(i * n_c, n_c), n_c), :] = flip[top:top + n_c].astype(BF16)
            t_ref[l, pl.ds(i, n_c, stride=I_STRIDE), :] = flip[top + n_c:top + 2 * n_c]
        return carry
    lax.fori_loop(0, n_i, columns, 0)
    for l in range(layers):
        for d in range(n_c):
            b_ref[l, d] = t_ref[l, d * I_STRIDE:d * I_STRIDE + n_i, :].astype(BF16)


def msa_project(msa_act, norm_w, w_bd, bias):
    seqs, n_i, n_m = msa_act.shape
    layers = norm_w.shape[0]
    n_c = w_bd.shape[1] // (2 * layers)
    s_blk = LANES
    return pl.pallas_call(
        msa_kernel, grid=(seqs // s_blk,),
        in_specs=[
            pl.BlockSpec((s_blk, n_i, n_m), lambda s: (s, 0, 0)),
            pl.BlockSpec(norm_w.shape, lambda s: (0, 0, 0)),
            pl.BlockSpec(w_bd.shape, lambda s: (0, 0)),
            pl.BlockSpec(bias.shape, lambda s: (0, 0)),
        ],
        out_specs=(pl.BlockSpec((layers, n_i * n_c, s_blk), lambda s: (0, 0, s)),
                   pl.BlockSpec((layers, n_c, n_i, s_blk), lambda s: (0, 0, 0, s))),
        out_shape=(jax.ShapeDtypeStruct((layers, n_i * n_c, seqs), BF16),
                   jax.ShapeDtypeStruct((layers, n_c, n_i, seqs), BF16)),
        scratch_shapes=[pltpu.VMEM((s_blk * I_STRIDE, w_bd.shape[1]), F32),
                        pltpu.VMEM((layers, n_c * I_STRIDE, s_blk), F32)],
        compiler_params=pltpu.CompilerParams(dimension_semantics=('arbitrary',)),
        cost_estimate=pl.CostEstimate(flops=2 * seqs * n_i * n_m * 2 * n_c * layers,
                                      bytes_accessed=2 * seqs * n_i * (n_m + 2 * n_c * layers), transcendentals=0),
        name='msa_project',
    )(msa_act, norm_w, w_bd, bias)


def opm_kernel(inv_s, first, last, a_ref, b_ref, w_ref, bias_ref, *rest):
    acc_ref, out_ref, q_ref = (None,) * first + rest
    part = pl.program_id(1)
    dev, d_blk, j_loc, seqs = b_ref.shape
    n_i, _, j_blk = q_ref.shape
    n_c = a_ref.shape[0] // n_i
    for d in range(d_blk):
        rhs = b_ref[:, d, :, :].reshape(dev * j_loc, seqs)
        prod = (dot_nt(a_ref[...], rhs) * inv_s).astype(BF16)
        base = pl.multiple_of((part * d_blk + d) * n_c, n_c)
        q_ref[:, pl.ds(base, n_c), :] = prod.reshape(n_i, n_c, j_blk)

    @pl.when(part == pl.num_programs(1) - 1)
    def _():
        def body(i, carry):
            upd = dot_nn(w_ref[...], q_ref[i])
            if not first:
                upd = acc_ref[i] + upd
            out_ref[i] = (upd + bias_ref[...]).astype(BF16) if last else upd
            return carry
        lax.fori_loop(0, n_i, body, 0)


def opm_update(a_t, b_all, w_t, bias, acc=None, last=True):
    n_dev, n_d, j_loc, seqs = b_all.shape
    rows_c = a_t.shape[0]
    n_z = w_t.shape[0]
    n_c = w_t.shape[1] // n_d
    n_i = rows_c // n_c
    cols = n_dev * j_loc
    j_blk = 2 * LANES
    dev_blk = j_blk // j_loc
    d_blk = math.gcd(n_d, 8)
    grid = (cols // j_blk, n_d // d_blk)
    row_spec = pl.BlockSpec((n_i, n_z, j_blk), lambda j, d: (0, 0, j))
    first = acc is None
    return pl.pallas_call(
        functools.partial(opm_kernel, 1.0 / seqs, first, last),
        grid=grid,
        in_specs=[
            pl.BlockSpec((rows_c, seqs), lambda j, d: (0, 0)),
            pl.BlockSpec((dev_blk, d_blk, j_loc, seqs), lambda j, d: (j, d, 0, 0)),
            pl.BlockSpec(w_t.shape, lambda j, d: (0, 0)),
            pl.BlockSpec(bias.shape, lambda j, d: (0, 0)),
        ] + ([] if first else [row_spec]),
        out_specs=row_spec,
        out_shape=jax.ShapeDtypeStruct((n_i, n_z, cols), BF16 if last else F32),
        scratch_shapes=[pltpu.VMEM((n_i, n_d * n_c, j_blk), BF16)],
        compiler_params=pltpu.CompilerParams(dimension_semantics=('arbitrary', 'arbitrary')),
        cost_estimate=pl.CostEstimate(
            flops=2 * rows_c * seqs * cols * n_d + 2 * n_i * cols * n_d * n_c * n_z,
            bytes_accessed=2 * (n_dev * n_d * j_loc * seqs + n_i * n_z * cols), transcendentals=0),
        name='opm_update',
    )(a_t, b_all, w_t, bias, *(() if first else (acc,)))


def norm_columns(x_f32, gain, offset):
    mean_val = jnp.mean(x_f32, axis=0, keepdims=True)
    centered = x_f32 - mean_val
    var_val = jnp.mean(centered * centered, axis=0, keepdims=True)
    return (centered * lax.rsqrt(var_val + LN_EPS) * gain + offset).astype(BF16)


def project_row(i, z_f32, mask_row, nin_ref, w_ref, b_ref, gate_ref, s_refs):
    zn = norm_columns(z_f32, nin_ref[0], nin_ref[1])
    n_z = z_f32.shape[0]
    lanes = z_f32.shape[1]
    gate_ref[i] = jax.nn.sigmoid(dot_nn(w_ref[4], zn) + b_ref[4])
    for q in range(2):
        lin = dot_nn(w_ref[2 * q], zn) + b_ref[2 * q]
        sig = jax.nn.sigmoid(dot_nn(w_ref[2 * q + 1], zn) + b_ref[2 * q + 1])
        val = mask_row * sig * lin
        for t in range(lanes // LANES):
            s_refs[q][t, pl.ds(i, n_z, stride=I_STRIDE), :] = val[:, t * LANES:(t + 1) * LANES]


def emit_ab(ab_ref, s_refs):
    n_dev, _, n_cl, n_i, lanes = ab_ref.shape

    def body(dev, carry):
        for q in range(2):
            for c in range(n_cl):
                base = pl.multiple_of((dev * n_cl + c) * I_STRIDE, 8)
                for t in range(lanes // LANES):
                    ab_ref[dev, q, c, :, t * LANES:(t + 1) * LANES] = s_refs[q][t, pl.ds(base, n_i), :].astype(BF16)
        return carry
    lax.fori_loop(0, n_dev, body, 0)


def start_kernel(z_ref, u_ref, mask_ref, nin_ref, w_ref, b_ref, z_out, gate_ref, ab_ref, s_a, s_b):
    n_i = z_ref.shape[0]

    def body(i, carry):
        z_new = (z_ref[i].astype(F32) + u_ref[i].astype(F32)).astype(BF16)
        z_out[i] = z_new
        project_row(i, z_new.astype(F32), mask_ref[pl.ds(i, 1), :], nin_ref, w_ref, b_ref, gate_ref, (s_a, s_b))
        return carry
    lax.fori_loop(0, n_i, body, 0)
    emit_ab(ab_ref, (s_a, s_b))


def finish_stats(o_ref, s_o):
    n_c, n_i, lanes = o_ref.shape
    mean_val = jnp.mean(o_ref[...], axis=0)
    centered = o_ref[...] - mean_val[None]
    var_val = jnp.mean(centered * centered, axis=0)
    rstd = lax.rsqrt(var_val + LN_EPS)

    def body(c, carry):
        base = pl.multiple_of(c * I_STRIDE, 8)
        norm = (o_ref[c] - mean_val) * rstd
        for t in range(lanes // LANES):
            s_o[t, pl.ds(base, n_i), :] = norm[:, t * LANES:(t + 1) * LANES]
        return carry
    lax.fori_loop(0, n_c, body, 0)


def finish_row(i, z_ref, gate_ref, nout_ref, wo_ref, bo_ref, s_o):
    tiles, rows, _ = s_o.shape
    n_c = rows // I_STRIDE
    norm = jnp.concatenate([s_o[t, pl.ds(i, n_c, stride=I_STRIDE), :] for t in range(tiles)], axis=1)
    norm = (norm * nout_ref[0] + nout_ref[1]).astype(BF16)
    upd = (dot_nn(wo_ref[...], norm) + bo_ref[...]).astype(BF16)
    return (z_ref[i].astype(F32) + gate_ref[i] * upd.astype(F32)).astype(BF16)


def middle_kernel(o_ref, zin_ref, gin_ref, nout_ref, wo_ref, bo_ref, u_ref, mask_ref, nin_ref, w_ref, b_ref,
                  z_out, gate_ref, ab_ref, s_a, s_b, s_o):
    n_i = zin_ref.shape[0]
    finish_stats(o_ref, s_o)

    def body(i, carry):
        z_mid = finish_row(i, zin_ref, gin_ref, nout_ref, wo_ref, bo_ref, s_o)
        z_new = (z_mid.astype(F32) + u_ref[i].astype(F32)).astype(BF16)
        z_out[i] = z_new
        project_row(i, z_new.astype(F32), mask_ref[pl.ds(i, 1), :], nin_ref, w_ref, b_ref, gate_ref, (s_a, s_b))
        return carry
    lax.fori_loop(0, n_i, body, 0)
    emit_ab(ab_ref, (s_a, s_b))


def end_kernel(o_ref, zin_ref, gin_ref, nout_ref, wo_ref, bo_ref, z_out, s_o):
    n_i = zin_ref.shape[0]
    finish_stats(o_ref, s_o)

    def body(i, carry):
        z_new = finish_row(i, zin_ref, gin_ref, nout_ref, wo_ref, bo_ref, s_o)
        z_out[i] = z_new.astype(F32).T.astype(BF16)
        return carry
    lax.fori_loop(0, n_i, body, 0)


J_BLK = 256


def tri_call(kind, n_dev, args):
    kernels = {'start': start_kernel, 'middle': middle_kernel, 'end': end_kernel}
    if kind == 'start':
        n_i, n_z, cols = args[0].shape
    else:
        n_i, n_z, cols = args[1].shape
    n_ch = n_z

    def blk(arr, which):
        shape = arr.shape
        if which == 'j':
            return pl.BlockSpec(shape[:-1] + (J_BLK,), lambda j: (0,) * (len(shape) - 1) + (j,))
        return pl.BlockSpec(shape, lambda j: (0,) * len(shape))

    tiles = J_BLK // LANES
    fin = ['j', 'j', 'j', 'w', 'w', 'w']
    pro = ['j', 'j', 'w', 'w', 'w']
    kinds = {'start': ['j'] + pro, 'middle': fin + pro, 'end': fin}[kind]
    scr = pltpu.VMEM((tiles, n_ch * I_STRIDE, LANES), F32)
    if kind == 'end':
        out_shape = jax.ShapeDtypeStruct((n_i, cols, n_z), BF16)
        out_specs = pl.BlockSpec((n_i, J_BLK, n_z), lambda j: (0, j, 0))
        scratch = [scr]
    else:
        out_shape = (jax.ShapeDtypeStruct((n_i, n_z, cols), BF16),
                     jax.ShapeDtypeStruct((n_i, n_z, cols), F32),
                     jax.ShapeDtypeStruct((n_dev, 2, n_ch // n_dev, n_i, cols), BF16))
        out_specs = tuple(blk(s, 'j') for s in out_shape)
        scratch = [scr, scr] + ([scr] if kind == 'middle' else [])
    return pl.pallas_call(
        kernels[kind], grid=(cols // J_BLK,),
        in_specs=[blk(a, k) for a, k in zip(args, kinds)],
        out_specs=out_specs, out_shape=out_shape, scratch_shapes=scratch,
        compiler_params=pltpu.CompilerParams(dimension_semantics=('arbitrary',)),
        cost_estimate=pl.CostEstimate(flops=12 * n_i * cols * n_z * n_z, bytes_accessed=16 * n_i * cols * n_z,
                                      transcendentals=3 * n_i * cols * n_z),
        name='tri_' + kind,
    )(*args)


def product_kernel(ab_ref, o_ref):
    n_dev, _, _, n_i, cols = ab_ref.shape
    left = ab_ref[:, 0, 0].reshape(n_dev * n_i, cols)
    right = ab_ref[:, 1, 0].reshape(n_dev * n_i, cols)
    half = cols // 2
    for h in range(2):
        o_ref[:, 0, :, h * half:(h + 1) * half] = dot_nt(left, right[h * half:(h + 1) * half]).reshape(n_dev, n_i, half)


def tri_product(ab):
    n_dev, _, n_cl, n_i, cols = ab.shape
    rows = n_dev * n_i
    return pl.pallas_call(
        product_kernel, grid=(n_cl,),
        in_specs=[pl.BlockSpec((n_dev, 2, 1, n_i, cols), lambda c: (0, 0, c, 0, 0))],
        out_specs=pl.BlockSpec((n_dev, 1, n_i, cols), lambda c: (0, c, 0, 0)),
        out_shape=jax.ShapeDtypeStruct((n_dev, n_cl, n_i, cols), F32),
        compiler_params=pltpu.CompilerParams(dimension_semantics=('arbitrary',)),
        cost_estimate=pl.CostEstimate(flops=2 * n_cl * rows * rows * cols, bytes_accessed=8 * n_cl * rows * cols,
                                      transcendentals=0),
        name='tri_product',
    )(ab)


def solution(mesh):
    pair_spec = P(('batch', 'dap'), None, None)
    mask_spec = P(('batch', 'dap'), None)
    msa_spec = P(None, ('batch', 'dap'), None)
    n_dev = mesh.shape['dap']

    def column(vec):
        return vec.astype(F32)[..., None]

    def device_fn(pair_act, pair_mask, msa_act, opm_norm, opm_w_in, opm_b_in, opm_w_out, opm_b_out, tri_norm_in, tri_w_ab, tri_b_ab, tri_w_gate, tri_b_gate, tri_norm_out, tri_w_out, tri_b_out):
        layers = opm_norm.shape[0]
        n_i, cols, n_z = pair_act.shape
        n_c = opm_w_in.shape[-1]
        mask_f = pair_mask.astype(F32)
        n_m = msa_act.shape[-1]
        w_bd = jnp.zeros((layers, n_m, layers, 2 * n_c), BF16)
        for l in range(layers):
            w_bd = w_bd.at[l, :, l].set(opm_w_in[l].reshape(n_m, 2 * n_c))
        left, right = msa_project(msa_act, opm_norm.astype(F32), w_bd.reshape(layers * n_m, layers * 2 * n_c),
                                  opm_b_in.astype(F32).reshape(1, -1))
        chunks = [AG_CHUNKS] + [1] * (layers - 1)
        gathered = []
        for l in range(layers):
            size = n_c // chunks[l]
            gathered.append([lax.all_gather(right[l, k * size:(k + 1) * size], 'dap', axis=0) for k in range(chunks[l])])
        updates = []
        for l in range(layers):
            w_t = opm_w_out[l].reshape(n_c, n_c, n_z).transpose(2, 1, 0).reshape(n_z, n_c * n_c)
            acc, part = None, n_c * n_c // chunks[l]
            for k in range(chunks[l]):
                acc = opm_update(left[l], gathered[l][k], w_t[:, k * part:(k + 1) * part], column(opm_b_out[l]), acc,
                                 last=k == chunks[l] - 1)
            updates.append(acc)
        z_t = jnp.swapaxes(pair_act, 1, 2)
        fin = None
        for l in range(layers):
            w_all = jnp.concatenate([tri_w_ab[l].transpose(1, 2, 0), tri_w_gate[l].T[None]], axis=0)
            b_all = column(jnp.concatenate([tri_b_ab[l], tri_b_gate[l][None]], axis=0))
            pro = (updates[l], mask_f, column(tri_norm_in[l]), w_all, b_all)
            if l == 0:
                z_t, gate, ab = tri_call('start', n_dev, (z_t,) + pro)
            else:
                z_t, gate, ab = tri_call('middle', n_dev, fin + pro)
            ab = lax.all_to_all(ab.reshape(n_dev, -1, cols), 'dap', 0, 0, tiled=True).reshape(ab.shape)
            prod = lax.all_to_all(tri_product(ab), 'dap', 0, 0, tiled=True)
            fin = (prod.reshape(-1, n_i, cols), z_t, gate, column(tri_norm_out[l]), tri_w_out[l].T, column(tri_b_out[l]))
        return tri_call('end', n_dev, fin)

    return jax.shard_map(device_fn, mesh=mesh, in_specs=(pair_spec, mask_spec, msa_spec) + (P(),) * 13, out_specs=pair_spec, check_vma=False)
```

```python
import functools
import math
import jax
import jax.numpy as jnp
from jax import lax
from jax.experimental import pallas as pl
from jax.experimental.pallas import tpu as pltpu
from jax.sharding import PartitionSpec as P

LN_EPS = 1e-5
LANES = 128
ROW_UNROLL = 4
F32 = jnp.float32
BF16 = jnp.bfloat16


def dot_nn(a, b):
    return lax.dot_general(a, b, (((1,), (0,)), ((), ())), preferred_element_type=F32)


def dot_nt(a, b):
    return lax.dot_general(a, b, (((1,), (1,)), ((), ())), preferred_element_type=F32)


I_STRIDE = 24
S_GROUP = 32


def msa_kernel(m_ref, norm_ref, w_ref, bias_ref, *refs):
    y_ref, t_ref = refs[-2:]
    layers = t_ref.shape[0]
    a_refs, b_refs = refs[:layers], refs[layers:2 * layers]
    s_blk, n_i, _ = m_ref.shape
    n_c = b_refs[0].shape[0]
    group = S_GROUP

    def rows(g, carry):
        base = pl.multiple_of(g * group, group)
        x = m_ref[pl.ds(base, group)].astype(F32).reshape(group * n_i, -1)
        mean_val = jnp.mean(x, axis=-1, keepdims=True)
        centered = x - mean_val
        var_val = jnp.mean(centered * centered, axis=-1, keepdims=True)
        scaled = centered * lax.rsqrt(var_val + LN_EPS)
        normed = jnp.concatenate([(scaled * norm_ref[l, 0:1] + norm_ref[l, 1:2]).astype(BF16) for l in range(layers)], axis=1)
        proj = dot_nn(normed, w_ref[...]) + bias_ref[...]
        for s in range(group):
            y_ref[pl.ds(pl.multiple_of((base + s) * I_STRIDE, 8), n_i), :] = proj[s * n_i:(s + 1) * n_i]
        return carry
    lax.fori_loop(0, s_blk // group, rows, 0, unroll=2)

    def columns(i, carry):
        flip = y_ref[pl.ds(i, s_blk, stride=I_STRIDE), :].T
        for l in range(layers):
            top = 2 * l * n_c
            a_refs[l][pl.ds(pl.multiple_of(i * n_c, n_c), n_c), :] = flip[top:top + n_c].astype(BF16)
            t_ref[l, pl.ds(i, n_c, stride=I_STRIDE), :] = flip[top + n_c:top + 2 * n_c]
        return carry
    lax.fori_loop(0, n_i, columns, 0, unroll=4)
    for l in range(layers):
        for d in range(n_c):
            b_refs[l][d] = t_ref[l, d * I_STRIDE:d * I_STRIDE + n_i, :].astype(BF16)


def msa_project(msa_act, norm_w, w_bd, bias):
    seqs, n_i, n_m = msa_act.shape
    layers = norm_w.shape[0]
    n_c = w_bd.shape[1] // (2 * layers)
    s_blk = LANES
    return pl.pallas_call(
        msa_kernel, grid=(seqs // s_blk,),
        in_specs=[
            pl.BlockSpec((s_blk, n_i, n_m), lambda s: (s, 0, 0)),
            pl.BlockSpec(norm_w.shape, lambda s: (0, 0, 0)),
            pl.BlockSpec(w_bd.shape, lambda s: (0, 0)),
            pl.BlockSpec(bias.shape, lambda s: (0, 0)),
        ],
        out_specs=(pl.BlockSpec((n_i * n_c, s_blk), lambda s: (0, s)),) * layers
        + (pl.BlockSpec((n_c, n_i, s_blk), lambda s: (0, 0, s)),) * layers,
        out_shape=(jax.ShapeDtypeStruct((n_i * n_c, seqs), BF16),) * layers
        + (jax.ShapeDtypeStruct((n_c, n_i, seqs), BF16),) * layers,
        scratch_shapes=[pltpu.VMEM((s_blk * I_STRIDE, w_bd.shape[1]), F32),
                        pltpu.VMEM((layers, n_c * I_STRIDE, s_blk), F32)],
        compiler_params=pltpu.CompilerParams(dimension_semantics=('arbitrary',)),
        cost_estimate=pl.CostEstimate(flops=2 * seqs * n_i * n_m * 2 * n_c * layers,
                                      bytes_accessed=2 * seqs * n_i * (n_m + 2 * n_c * layers), transcendentals=0),
        name='msa_project',
    )(msa_act, norm_w, w_bd, bias)


def opm_kernel(inv_s, first, last, a_ref, b_ref, w_ref, bias_ref, *rest):
    acc_ref, out_ref, q_ref = (None,) * first + rest
    part = pl.program_id(1)
    dev, d_blk, j_loc, seqs = b_ref.shape
    n_i, _, j_blk = q_ref.shape
    n_c = a_ref.shape[0] // n_i
    for d in range(d_blk):
        rhs = b_ref[:, d, :, :].reshape(dev * j_loc, seqs)
        prod = (dot_nt(a_ref[...], rhs) * inv_s).astype(BF16)
        base = pl.multiple_of((part * d_blk + d) * n_c, n_c)
        q_ref[:, pl.ds(base, n_c), :] = prod.reshape(n_i, n_c, j_blk)

    @pl.when(part == pl.num_programs(1) - 1)
    def _():
        def body(i, carry):
            upd = dot_nn(w_ref[...], q_ref[i])
            if not first:
                upd = acc_ref[i] + upd
            out_ref[i] = (upd + bias_ref[...]).astype(BF16) if last else upd
            return carry
        lax.fori_loop(0, n_i, body, 0, unroll=4)


def opm_update(a_t, b_all, w_t, bias, acc=None, last=True):
    n_dev, n_d, j_loc, seqs = b_all.shape
    rows_c = a_t.shape[0]
    n_z = w_t.shape[0]
    n_c = w_t.shape[1] // n_d
    n_i = rows_c // n_c
    cols = n_dev * j_loc
    j_blk = 2 * LANES
    dev_blk = j_blk // j_loc
    d_blk = math.gcd(n_d, 8)
    grid = (cols // j_blk, n_d // d_blk)
    row_spec = pl.BlockSpec((n_i, n_z, j_blk), lambda j, d: (0, 0, j))
    first = acc is None
    return pl.pallas_call(
        functools.partial(opm_kernel, 1.0 / seqs, first, last),
        grid=grid,
        in_specs=[
            pl.BlockSpec((rows_c, seqs), lambda j, d: (0, 0)),
            pl.BlockSpec((dev_blk, d_blk, j_loc, seqs), lambda j, d: (j, d, 0, 0)),
            pl.BlockSpec(w_t.shape, lambda j, d: (0, 0)),
            pl.BlockSpec(bias.shape, lambda j, d: (0, 0)),
        ] + ([] if first else [row_spec]),
        out_specs=row_spec,
        out_shape=jax.ShapeDtypeStruct((n_i, n_z, cols), BF16 if last else F32),
        scratch_shapes=[pltpu.VMEM((n_i, n_d * n_c, j_blk), BF16)],
        compiler_params=pltpu.CompilerParams(dimension_semantics=('arbitrary', 'arbitrary')),
        cost_estimate=pl.CostEstimate(
            flops=2 * rows_c * seqs * cols * n_d + 2 * n_i * cols * n_d * n_c * n_z,
            bytes_accessed=2 * (n_dev * n_d * j_loc * seqs + n_i * n_z * cols), transcendentals=0),
        name='opm_update',
    )(a_t, b_all, w_t, bias, *(() if first else (acc,)))


def norm_columns(x_f32, gain, offset):
    mean_val = jnp.mean(x_f32, axis=0, keepdims=True)
    centered = x_f32 - mean_val
    var_val = jnp.mean(centered * centered, axis=0, keepdims=True)
    return (centered * lax.rsqrt(var_val + LN_EPS) * gain + offset).astype(BF16)


def sigmoid(x):
    return 0.5 * jnp.tanh(0.5 * x) + 0.5


def project_row(i, z_f32, mask_row, nin_ref, w_ref, b_ref, s_refs):
    zn = norm_columns(z_f32, nin_ref[0], nin_ref[1])
    n_z, lanes = z_f32.shape
    n_ch = w_ref.shape[0] // 4
    proj = dot_nn(w_ref[...], zn) + b_ref[...]
    for q in range(2):
        lin = proj[2 * q * n_ch:(2 * q + 1) * n_ch]
        sig = sigmoid(proj[(2 * q + 1) * n_ch:(2 * q + 2) * n_ch])
        val = mask_row * sig * lin
        for t in range(lanes // LANES):
            s_refs[q][t, pl.ds(i, n_ch, stride=I_STRIDE), :] = val[:, t * LANES:(t + 1) * LANES]


def gate_kernel(z_ref, nin_ref, w_ref, b_ref, gate_ref):
    def body(i, carry):
        zn = norm_columns(z_ref[i].astype(F32), nin_ref[0], nin_ref[1])
        gate_ref[i] = sigmoid(dot_nn(w_ref[...], zn) + b_ref[...])
        return carry
    lax.fori_loop(0, z_ref.shape[0], body, 0, unroll=4)


def gate_call(z_t, norm_in, w_gate, b_gate):
    n_i, n_z, cols = z_t.shape
    row_spec = pl.BlockSpec((n_i, n_z, J_BLK), lambda j: (0, 0, j))
    return pl.pallas_call(
        gate_kernel, grid=(cols // J_BLK,),
        in_specs=[row_spec, pl.BlockSpec(norm_in.shape, lambda j: (0, 0, 0)), pl.BlockSpec(w_gate.shape, lambda j: (0, 0)),
                  pl.BlockSpec(b_gate.shape, lambda j: (0, 0))],
        out_specs=row_spec, out_shape=jax.ShapeDtypeStruct(z_t.shape, F32),
        compiler_params=pltpu.CompilerParams(dimension_semantics=('arbitrary',)),
        cost_estimate=pl.CostEstimate(flops=12 * n_i * cols * n_z * n_z, bytes_accessed=6 * n_i * cols * n_z,
                                      transcendentals=n_i * cols * n_z),
        name='tri_gate',
    )(z_t, norm_in, w_gate, b_gate)


def emit_ab(ab_ref, s_refs):
    n_dev, _, n_cl, n_i, lanes = ab_ref.shape

    def body(dev, carry):
        for q in range(2):
            for c in range(n_cl):
                base = pl.multiple_of((dev * n_cl + c) * I_STRIDE, 8)
                for t in range(lanes // LANES):
                    ab_ref[dev, q, c, :, t * LANES:(t + 1) * LANES] = s_refs[q][t, pl.ds(base, n_i), :].astype(BF16)
        return carry
    lax.fori_loop(0, n_dev, body, 0, unroll=2)


def start_kernel(z_ref, u_ref, mask_ref, nin_ref, w_ref, b_ref, z_out, ab_ref, s_a, s_b):
    n_i = z_ref.shape[0]

    def body(i, carry):
        z_new = (z_ref[i].astype(F32) + u_ref[i].astype(F32)).astype(BF16)
        z_out[i] = z_new
        project_row(i, z_new.astype(F32), mask_ref[pl.ds(i, 1), :], nin_ref, w_ref, b_ref, (s_a, s_b))
        return carry
    lax.fori_loop(0, n_i, body, 0, unroll=ROW_UNROLL)
    emit_ab(ab_ref, (s_a, s_b))


def finish_stats(o_ref, s_o, r_ref):
    n_c, n_i, lanes = o_ref.shape
    total = lax.fori_loop(0, n_c, lambda c, acc: acc + o_ref[c], jnp.zeros((n_i, lanes), F32), unroll=16)
    mean_val = total / n_c

    def body(c, acc):
        base = pl.multiple_of(c * I_STRIDE, 8)
        centered = o_ref[c] - mean_val
        for t in range(lanes // LANES):
            s_o[t, pl.ds(base, n_i), :] = centered[:, t * LANES:(t + 1) * LANES]
        return acc + centered * centered
    square = lax.fori_loop(0, n_c, body, jnp.zeros((n_i, lanes), F32), unroll=16)
    r_ref[...] = lax.rsqrt(square / n_c + LN_EPS)


def finish_row(i, z_ref, gate_ref, nout_ref, wo_ref, bo_ref, s_o, r_ref):
    tiles, rows, _ = s_o.shape
    n_c = rows // I_STRIDE
    centered = jnp.concatenate([s_o[t, pl.ds(i, n_c, stride=I_STRIDE), :] for t in range(tiles)], axis=1)
    norm = (centered * r_ref[pl.ds(i, 1), :] * nout_ref[0] + nout_ref[1]).astype(BF16)
    upd = (dot_nn(wo_ref[...], norm) + bo_ref[...]).astype(BF16)
    return (z_ref[i].astype(F32) + gate_ref[i] * upd.astype(F32)).astype(BF16)


def middle_kernel(o_ref, zin_ref, gin_ref, nout_ref, wo_ref, bo_ref, u_ref, mask_ref, nin_ref, w_ref, b_ref,
                  z_out, ab_ref, s_a, s_b, s_o, r_ref):
    n_i = zin_ref.shape[0]
    finish_stats(o_ref, s_o, r_ref)

    def body(i, carry):
        z_mid = finish_row(i, zin_ref, gin_ref, nout_ref, wo_ref, bo_ref, s_o, r_ref)
        z_new = (z_mid.astype(F32) + u_ref[i].astype(F32)).astype(BF16)
        z_out[i] = z_new
        project_row(i, z_new.astype(F32), mask_ref[pl.ds(i, 1), :], nin_ref, w_ref, b_ref, (s_a, s_b))
        return carry
    lax.fori_loop(0, n_i, body, 0, unroll=ROW_UNROLL)
    emit_ab(ab_ref, (s_a, s_b))


def end_kernel(o_ref, zin_ref, gin_ref, nout_ref, wo_ref, bo_ref, z_out, s_o, r_ref):
    n_i = zin_ref.shape[0]
    finish_stats(o_ref, s_o, r_ref)

    def body(i, carry):
        z_new = finish_row(i, zin_ref, gin_ref, nout_ref, wo_ref, bo_ref, s_o, r_ref)
        z_out[i] = z_new.astype(F32).T.astype(BF16)
        return carry
    lax.fori_loop(0, n_i, body, 0, unroll=ROW_UNROLL)


J_BLK = 256


def tri_call(kind, n_dev, args):
    kernels = {'start': start_kernel, 'middle': middle_kernel, 'end': end_kernel}
    if kind == 'start':
        n_i, n_z, cols = args[0].shape
    else:
        n_i, n_z, cols = args[1].shape
    n_ch = n_z

    def blk(arr, which):
        shape = arr.shape
        if which == 'j':
            return pl.BlockSpec(shape[:-1] + (J_BLK,), lambda j: (0,) * (len(shape) - 1) + (j,))
        return pl.BlockSpec(shape, lambda j: (0,) * len(shape))

    tiles = J_BLK // LANES
    fin = ['j', 'j', 'j', 'w', 'w', 'w']
    pro = ['j', 'j', 'w', 'w', 'w']
    kinds = {'start': ['j'] + pro, 'middle': fin + pro, 'end': fin}[kind]
    scr = pltpu.VMEM((tiles, n_ch * I_STRIDE, LANES), F32)
    stat = pltpu.VMEM((n_i, J_BLK), F32)
    if kind == 'end':
        out_shape = jax.ShapeDtypeStruct((n_i, cols, n_z), BF16)
        out_specs = pl.BlockSpec((n_i, J_BLK, n_z), lambda j: (0, j, 0))
        scratch = [scr, stat]
    else:
        out_shape = (jax.ShapeDtypeStruct((n_i, n_z, cols), BF16),
                     jax.ShapeDtypeStruct((n_dev, 2, n_ch // n_dev, n_i, cols), BF16))
        out_specs = tuple(blk(s, 'j') for s in out_shape)
        scratch = [scr, scr] + ([scr, stat] if kind == 'middle' else [])
    return pl.pallas_call(
        kernels[kind], grid=(cols // J_BLK,),
        in_specs=[blk(a, k) for a, k in zip(args, kinds)],
        out_specs=out_specs, out_shape=out_shape, scratch_shapes=scratch,
        compiler_params=pltpu.CompilerParams(dimension_semantics=('arbitrary',)),
        cost_estimate=pl.CostEstimate(flops=12 * n_i * cols * n_z * n_z, bytes_accessed=16 * n_i * cols * n_z,
                                      transcendentals=3 * n_i * cols * n_z),
        name='tri_' + kind,
    )(*args)


def product_kernel(ab_ref, o_ref):
    n_dev, _, _, n_i, cols = ab_ref.shape
    left = ab_ref[:, 0, 0].reshape(n_dev * n_i, cols)
    right = ab_ref[:, 1, 0].reshape(n_dev * n_i, cols)
    half = cols // 2
    for h in range(2):
        o_ref[:, 0, :, h * half:(h + 1) * half] = dot_nt(left, right[h * half:(h + 1) * half]).reshape(n_dev, n_i, half)


def tri_product(ab):
    n_dev, _, n_cl, n_i, cols = ab.shape
    rows = n_dev * n_i
    return pl.pallas_call(
        product_kernel, grid=(n_cl,),
        in_specs=[pl.BlockSpec((n_dev, 2, 1, n_i, cols), lambda c: (0, 0, c, 0, 0))],
        out_specs=pl.BlockSpec((n_dev, 1, n_i, cols), lambda c: (0, c, 0, 0)),
        out_shape=jax.ShapeDtypeStruct((n_dev, n_cl, n_i, cols), F32),
        compiler_params=pltpu.CompilerParams(dimension_semantics=('arbitrary',)),
        cost_estimate=pl.CostEstimate(flops=2 * n_cl * rows * rows * cols, bytes_accessed=8 * n_cl * rows * cols,
                                      transcendentals=0),
        name='tri_product',
    )(ab)


def solution(mesh):
    pair_spec = P(('batch', 'dap'), None, None)
    mask_spec = P(('batch', 'dap'), None)
    msa_spec = P(None, ('batch', 'dap'), None)
    n_dev = mesh.shape['dap']

    def column(vec):
        return vec.astype(F32)[..., None]

    def device_fn(pair_act, pair_mask, msa_act, opm_norm, opm_w_in, opm_b_in, opm_w_out, opm_b_out, tri_norm_in, tri_w_ab, tri_b_ab, tri_w_gate, tri_b_gate, tri_norm_out, tri_w_out, tri_b_out):
        layers = opm_norm.shape[0]
        n_i, cols, n_z = pair_act.shape
        n_c = opm_w_in.shape[-1]
        mask_f = pair_mask.astype(F32)
        n_m = msa_act.shape[-1]
        w_bd = jnp.zeros((layers, n_m, layers, 2 * n_c), BF16)
        for l in range(layers):
            w_bd = w_bd.at[l, :, l].set(opm_w_in[l].reshape(n_m, 2 * n_c))
        sides = msa_project(msa_act, opm_norm.astype(F32), w_bd.reshape(layers * n_m, layers * 2 * n_c),
                                  opm_b_in.astype(F32).reshape(1, -1))
        left, right = sides[:layers], sides[layers:]
        gathered = [lax.all_gather(r, 'dap', axis=0, tiled=True).reshape((n_dev,) + r.shape) for r in right]
        updates = []
        for l in range(layers):
            w_t = opm_w_out[l].reshape(n_c, n_c, n_z).transpose(2, 1, 0).reshape(n_z, n_c * n_c)
            updates.append(opm_update(left[l], gathered[l], w_t, column(opm_b_out[l])))
        z_t = jnp.swapaxes(pair_act, 1, 2)
        fin = None
        for l in range(layers):
            w_all = tri_w_ab[l].transpose(1, 2, 0).reshape(-1, n_z)
            norm_in = column(tri_norm_in[l])
            pro = (updates[l], mask_f, norm_in, w_all, column(tri_b_ab[l].reshape(-1)))
            if l == 0:
                z_t, ab = tri_call('start', n_dev, (z_t,) + pro)
            else:
                z_t, ab = tri_call('middle', n_dev, fin + pro)
            ab = lax.all_to_all(ab.reshape(n_dev, -1, cols), 'dap', 0, 0, tiled=True).reshape(ab.shape)
            prod, z_g = lax.optimization_barrier((tri_product(ab), z_t))
            gate = gate_call(z_g, norm_in, tri_w_gate[l].T, column(tri_b_gate[l]))
            prod = lax.all_to_all(prod, 'dap', 0, 0, tiled=True)
            fin = (prod.reshape(-1, n_i, cols), z_t, gate, column(tri_norm_out[l]), tri_w_out[l].T, column(tri_b_out[l]))
        return tri_call('end', n_dev, fin)

    return jax.shard_map(device_fn, mesh=mesh, in_specs=(pair_spec, mask_spec, msa_spec) + (P(),) * 13, out_specs=pair_spec, check_vma=False)
```

```python
import functools
import math
import jax
import jax.numpy as jnp
from jax import lax
from jax.experimental import pallas as pl
from jax.experimental.pallas import tpu as pltpu
from jax.sharding import PartitionSpec as P

LN_EPS = 1e-5
LANES = 128
ROW_UNROLL = 4
F32 = jnp.float32
BF16 = jnp.bfloat16


def dot_nn(a, b):
    return lax.dot_general(a, b, (((1,), (0,)), ((), ())), preferred_element_type=F32)


def dot_nt(a, b):
    return lax.dot_general(a, b, (((1,), (1,)), ((), ())), preferred_element_type=F32)


I_STRIDE = 24
S_GROUP = 32


def msa_kernel(m_ref, norm_ref, w_ref, bias_ref, *refs):
    y_ref, t_ref = refs[-2:]
    layers = t_ref.shape[0]
    a_refs, b_refs = refs[:layers], refs[layers:2 * layers]
    s_blk, n_i, _ = m_ref.shape
    n_c = b_refs[0].shape[0]
    group = S_GROUP

    def rows(g, carry):
        base = pl.multiple_of(g * group, group)
        x = m_ref[pl.ds(base, group)].astype(F32).reshape(group * n_i, -1)
        mean_val = jnp.mean(x, axis=-1, keepdims=True)
        centered = x - mean_val
        var_val = jnp.mean(centered * centered, axis=-1, keepdims=True)
        scaled = centered * lax.rsqrt(var_val + LN_EPS)
        normed = jnp.concatenate([(scaled * norm_ref[l, 0:1] + norm_ref[l, 1:2]).astype(BF16) for l in range(layers)], axis=1)
        proj = dot_nn(normed, w_ref[...]) + bias_ref[...]
        for s in range(group):
            y_ref[pl.ds(pl.multiple_of((base + s) * I_STRIDE, 8), n_i), :] = proj[s * n_i:(s + 1) * n_i]
        return carry
    lax.fori_loop(0, s_blk // group, rows, 0, unroll=2)

    def columns(i, carry):
        flip = y_ref[pl.ds(i, s_blk, stride=I_STRIDE), :].T
        for l in range(layers):
            top = 2 * l * n_c
            a_refs[l][pl.ds(pl.multiple_of(i * n_c, n_c), n_c), :] = flip[top:top + n_c].astype(BF16)
            t_ref[l, pl.ds(i, n_c, stride=I_STRIDE), :] = flip[top + n_c:top + 2 * n_c]
        return carry
    lax.fori_loop(0, n_i, columns, 0, unroll=4)
    for l in range(layers):
        for d in range(n_c):
            b_refs[l][d] = t_ref[l, d * I_STRIDE:d * I_STRIDE + n_i, :].astype(BF16)


def msa_project(msa_act, norm_w, w_bd, bias):
    seqs, n_i, n_m = msa_act.shape
    layers = norm_w.shape[0]
    n_c = w_bd.shape[1] // (2 * layers)
    s_blk = LANES
    return pl.pallas_call(
        msa_kernel, grid=(seqs // s_blk,),
        in_specs=[
            pl.BlockSpec((s_blk, n_i, n_m), lambda s: (s, 0, 0)),
            pl.BlockSpec(norm_w.shape, lambda s: (0, 0, 0)),
            pl.BlockSpec(w_bd.shape, lambda s: (0, 0)),
            pl.BlockSpec(bias.shape, lambda s: (0, 0)),
        ],
        out_specs=(pl.BlockSpec((n_i * n_c, s_blk), lambda s: (0, s)),) * layers
        + (pl.BlockSpec((n_c, n_i, s_blk), lambda s: (0, 0, s)),) * layers,
        out_shape=(jax.ShapeDtypeStruct((n_i * n_c, seqs), BF16),) * layers
        + (jax.ShapeDtypeStruct((n_c, n_i, seqs), BF16),) * layers,
        scratch_shapes=[pltpu.VMEM((s_blk * I_STRIDE, w_bd.shape[1]), F32),
                        pltpu.VMEM((layers, n_c * I_STRIDE, s_blk), F32)],
        compiler_params=pltpu.CompilerParams(dimension_semantics=('arbitrary',)),
        cost_estimate=pl.CostEstimate(flops=2 * seqs * n_i * n_m * 2 * n_c * layers,
                                      bytes_accessed=2 * seqs * n_i * (n_m + 2 * n_c * layers), transcendentals=0),
        name='msa_project',
    )(msa_act, norm_w, w_bd, bias)


def opm_kernel(inv_s, first, last, a_ref, b_ref, w_ref, bias_ref, *rest):
    acc_ref, out_ref, q_ref = (None,) * first + rest
    part = pl.program_id(1)
    dev, d_blk, j_loc, seqs = b_ref.shape
    n_i, _, j_blk = q_ref.shape
    n_c = a_ref.shape[0] // n_i
    for d in range(d_blk):
        rhs = b_ref[:, d, :, :].reshape(dev * j_loc, seqs)
        prod = (dot_nt(a_ref[...], rhs) * inv_s).astype(BF16)
        base = pl.multiple_of((part * d_blk + d) * n_c, n_c)
        q_ref[:, pl.ds(base, n_c), :] = prod.reshape(n_i, n_c, j_blk)

    @pl.when(part == pl.num_programs(1) - 1)
    def _():
        def body(i, carry):
            upd = dot_nn(w_ref[...], q_ref[i])
            if not first:
                upd = acc_ref[i] + upd
            out_ref[i] = (upd + bias_ref[...]).astype(BF16) if last else upd
            return carry
        lax.fori_loop(0, n_i, body, 0, unroll=4)


def opm_update(a_t, b_all, w_t, bias, acc=None, last=True):
    n_dev, n_d, j_loc, seqs = b_all.shape
    rows_c = a_t.shape[0]
    n_z = w_t.shape[0]
    n_c = w_t.shape[1] // n_d
    n_i = rows_c // n_c
    cols = n_dev * j_loc
    j_blk = 2 * LANES
    dev_blk = j_blk // j_loc
    d_blk = math.gcd(n_d, 8)
    grid = (cols // j_blk, n_d // d_blk)
    row_spec = pl.BlockSpec((n_i, n_z, j_blk), lambda j, d: (0, 0, j))
    first = acc is None
    return pl.pallas_call(
        functools.partial(opm_kernel, 1.0 / seqs, first, last),
        grid=grid,
        in_specs=[
            pl.BlockSpec((rows_c, seqs), lambda j, d: (0, 0)),
            pl.BlockSpec((dev_blk, d_blk, j_loc, seqs), lambda j, d: (j, d, 0, 0)),
            pl.BlockSpec(w_t.shape, lambda j, d: (0, 0)),
            pl.BlockSpec(bias.shape, lambda j, d: (0, 0)),
        ] + ([] if first else [row_spec]),
        out_specs=row_spec,
        out_shape=jax.ShapeDtypeStruct((n_i, n_z, cols), BF16 if last else F32),
        scratch_shapes=[pltpu.VMEM((n_i, n_d * n_c, j_blk), BF16)],
        compiler_params=pltpu.CompilerParams(dimension_semantics=('arbitrary', 'arbitrary')),
        cost_estimate=pl.CostEstimate(
            flops=2 * rows_c * seqs * cols * n_d + 2 * n_i * cols * n_d * n_c * n_z,
            bytes_accessed=2 * (n_dev * n_d * j_loc * seqs + n_i * n_z * cols), transcendentals=0),
        name='opm_update',
    )(a_t, b_all, w_t, bias, *(() if first else (acc,)))


MESH_ID = pl.DeviceIdType.MESH
AG_UNITS = 4


class RingGather:
    def __init__(self, n, axis, src_ref, out_ref, r_sem, p_sem, s_sem, l_sem):
        self.n, self.side, self.axis = n, math.isqrt(n // 2), axis
        self.src, self.out = src_ref, out_ref
        self.r_sem, self.p_sem, self.s_sem, self.l_sem = r_sem, p_sem, s_sem, l_sem
        me = lax.axis_index(axis)
        self.me, self.core = me, me % 2
        self.x, self.y = (me // 2) % self.side, me // (2 * self.side)
        self.size = src_ref.shape[0] // AG_UNITS

    def at(self, u, k1, k2, other=False):
        kx, ky = (k1, k2) if u < AG_UNITS // 2 else (k2, k1)
        core = 1 - self.core if other else self.core
        return (((self.y + ky) % self.side) * self.side + (self.x + kx) % self.side) * 2 + core

    def neighbours(self):
        last = self.side - 1
        return [self.at(0, 1, 0), self.at(0, last, 0), self.at(0, 0, 1), self.at(0, 0, last), self.at(0, 0, 0, True)]

    def barrier(self):
        sem = pltpu.get_barrier_semaphore()
        peers = self.neighbours()
        for p in peers:
            pl.semaphore_signal(sem, inc=1, device_id={self.axis: p}, device_id_type=MESH_ID)
        pl.semaphore_wait(sem, len(peers))

    def copy(self, u, k1, k2, way):
        rows = pl.ds(u * self.size, self.size)
        owner = self.at(u, k1, k2)
        src = self.src.at[rows] if (k1, k2) == (0, 0) else self.out.at[owner, rows]
        step = (1, self.side - 1)[way % 2]
        if way < 2:
            dest, rk, sems = self.at(u, step, 0), ((k1 - step) % self.side, k2), self.r_sem
        elif way < 4:
            dest, rk, sems = self.at(u, 0, step), (k1, (k2 - step) % self.side), self.r_sem
        else:
            dest, rk, sems = self.at(u, 0, 0, True), (k1, k2), self.p_sem
        return pltpu.make_async_remote_copy(src, self.out.at[owner, rows], self.s_sem.at[u, k1, k2, way], sems.at[u, rk[0], rk[1]],
                                            device_id={self.axis: dest}, device_id_type=MESH_ID)

    def ways(self, u, k1, k2):
        last = self.side - 1
        plus = u % 2 == 0
        out = []
        if k2 == 0:
            if k1 == 0:
                out += [0, 1]
            elif k1 == last and plus:
                out.append(0)
            elif k1 == 1 and not plus:
                out.append(1)
            out += [2, 3]
        elif k2 == last and plus:
            out.append(2)
        elif k2 == 1 and not plus:
            out.append(3)
        return out + [4]

    def arrived(self, u, k1, k2, sems, other=False):
        rows = pl.ds(u * self.size, self.size)
        dst = self.out.at[self.at(u, k1, k2, other), rows]
        pltpu.make_async_remote_copy(dst, dst, self.s_sem.at[u, k1, k2, 4], sems.at[u, k1, k2],
                                     device_id={self.axis: self.at(0, 0, 0, True)}, device_id_type=MESH_ID).wait_recv()

    def steps(self):
        last = self.side - 1
        units = range(AG_UNITS)
        own = pltpu.make_async_copy(self.src, self.out.at[self.me], self.l_sem)

        def begin():
            own.start()
            for pair in ((0, 1), (2, 3), (4,)):
                for u in units:
                    for way in pair:
                        self.copy(u, 0, 0, way).start()

        def relay(k1, k2):
            for u in units:
                self.arrived(u, k1, k2, self.r_sem)
                for way in self.ways(u, k1, k2):
                    self.copy(u, k1, k2, way).start()

        def finish():
            for k1 in range(self.side):
                for k2 in range(self.side):
                    for u in units:
                        self.arrived(u, k1, k2, self.p_sem, True)
            for k1 in range(self.side):
                for k2 in range(self.side):
                    for u in units:
                        for way in self.ways(u, k1, k2):
                            self.copy(u, k1, k2, way).wait_send()
            own.wait()
        order = [(last, 0), (1, 0), (0, last), (0, 1), (2, 0)]
        order += [(k1, k2) for k1 in (last, 1, 2) for k2 in (last, 1)]
        order += [(k1, 2) for k1 in (0, last, 1, 2)]
        return [begin] + [functools.partial(relay, *o) for o in order] + [finish]


def gather_kernel(n, axis, src_ref, out_ref, *sems):
    ring = RingGather(n, axis, src_ref, out_ref, *sems)
    ring.barrier()
    for step in ring.steps():
        step()


def gather_scratch(side):
    dma = pltpu.SemaphoreType.DMA
    return [dma((AG_UNITS, side, side)), dma((AG_UNITS, side, side)), dma((AG_UNITS, side, side, 5)), dma]


def ring_gather(block, n, axis, cid):
    side = math.isqrt(n // 2)
    assert 2 * side * side == n and side == 4
    return pl.pallas_call(
        functools.partial(gather_kernel, n, axis),
        out_shape=jax.ShapeDtypeStruct((n,) + block.shape, block.dtype),
        in_specs=[pl.BlockSpec(memory_space=pl.ANY)], out_specs=pl.BlockSpec(memory_space=pl.ANY),
        scratch_shapes=gather_scratch(side),
        compiler_params=pltpu.CompilerParams(collective_id=cid, has_side_effects=True),
        name='ring_gather',
    )(block)


def gather_opm_kernel(n, axis, inv_s, src_ref, a_ref, b_ref, w_ref, bias_ref, out_ref, upd_ref, buf, q_ref, b_sem, *sems):
    ring = RingGather(n, axis, src_ref, out_ref, *sems)
    _, dev_blk, d_blk, j_loc, seqs = buf.shape
    n_i, _, j_blk = q_ref.shape
    n_c = a_ref.shape[0] // n_i
    parts = b_ref.shape[1] // d_blk
    total = (b_ref.shape[0] // dev_blk) * parts

    def load(k):
        j, part = k // parts, k % parts
        return pltpu.make_async_copy(b_ref.at[pl.ds(j * dev_blk, dev_blk), pl.ds(part * d_blk, d_blk)], buf.at[k % 2], b_sem.at[k % 2])

    def outer(k):
        if k + 1 < total:
            load(k + 1).start()
        load(k).wait()

        def body(d, carry):
            rhs = buf[k % 2, :, d].reshape(dev_blk * j_loc, seqs)
            prod = (dot_nt(a_ref[...], rhs) * inv_s).astype(BF16)
            base = pl.multiple_of(((k % parts) * d_blk + d) * n_c, n_c)
            q_ref[:, pl.ds(base, n_c), :] = prod.reshape(n_i, n_c, j_blk)
            return carry
        lax.fori_loop(0, d_blk, body, 0, unroll=2)

    def contract(j, low, high):
        def body(i, carry):
            upd = dot_nn(w_ref[...], q_ref[i]) + bias_ref[...]
            upd_ref[i, :, j * j_blk:(j + 1) * j_blk] = upd.astype(BF16)
            return carry
        lax.fori_loop(low, high, body, 0, unroll=4)
    pieces = []
    for k in range(total):
        pieces.append(functools.partial(outer, k))
        if k % parts == parts - 1:
            for half in range(2):
                pieces.append(functools.partial(contract, k // parts, half * n_i // 2, (half + 1) * n_i // 2))
    load(0).start()
    ring.barrier()
    steps = ring.steps()
    for k, step in enumerate(steps[:-1]):
        step()
        if k < len(pieces):
            pieces[k]()
    for piece in pieces[len(steps) - 1:]:
        piece()
    steps[-1]()


def gather_with_opm(block, n, axis, cid, a_t, b_all, w_t, bias):
    n_dev, n_d, j_loc, seqs = b_all.shape
    n_z = w_t.shape[0]
    n_c = w_t.shape[1] // n_d
    n_i = a_t.shape[0] // n_c
    cols = n_dev * j_loc
    j_blk = 2 * LANES
    d_blk = math.gcd(n_d, 8)
    side = math.isqrt(n // 2)
    assert 2 * side * side == n and side == 4
    any_spec = pl.BlockSpec(memory_space=pl.ANY)
    vmem_spec = pl.BlockSpec(memory_space=pltpu.VMEM)
    return pl.pallas_call(
        functools.partial(gather_opm_kernel, n, axis, 1.0 / seqs),
        out_shape=(jax.ShapeDtypeStruct((n,) + block.shape, block.dtype), jax.ShapeDtypeStruct((n_i, n_z, cols), BF16)),
        in_specs=[any_spec, vmem_spec, any_spec, vmem_spec, vmem_spec], out_specs=(any_spec, vmem_spec),
        scratch_shapes=[pltpu.VMEM((2, j_blk // j_loc, d_blk, j_loc, seqs), BF16), pltpu.VMEM((n_i, n_d * n_c, j_blk), BF16),
                        pltpu.SemaphoreType.DMA((2,))] + gather_scratch(side),
        compiler_params=pltpu.CompilerParams(collective_id=cid, has_side_effects=True),
        cost_estimate=pl.CostEstimate(flops=2 * a_t.shape[0] * seqs * cols * n_d * 4, bytes_accessed=2 * b_all.size, transcendentals=0),
        name='ring_gather_opm',
    )(block, a_t, b_all, w_t, bias)


def norm_columns(x_f32, gain, offset):
    mean_val = jnp.mean(x_f32, axis=0, keepdims=True)
    centered = x_f32 - mean_val
    var_val = jnp.mean(centered * centered, axis=0, keepdims=True)
    return (centered * lax.rsqrt(var_val + LN_EPS) * gain + offset).astype(BF16)


def sigmoid(x):
    return 0.5 * jnp.tanh(0.5 * x) + 0.5


def project_row(i, z_f32, mask_row, nin_ref, w_ref, b_ref, s_refs):
    zn = norm_columns(z_f32, nin_ref[0], nin_ref[1])
    n_z, lanes = z_f32.shape
    n_ch = w_ref.shape[0] // 4
    proj = dot_nn(w_ref[...], zn) + b_ref[...]
    for q in range(2):
        lin = proj[2 * q * n_ch:(2 * q + 1) * n_ch]
        sig = sigmoid(proj[(2 * q + 1) * n_ch:(2 * q + 2) * n_ch])
        val = mask_row * sig * lin
        for t in range(lanes // LANES):
            s_refs[q][t, pl.ds(i, n_ch, stride=I_STRIDE), :] = val[:, t * LANES:(t + 1) * LANES]


def gate_kernel(z_ref, nin_ref, w_ref, b_ref, gate_ref):
    def body(i, carry):
        zn = norm_columns(z_ref[i].astype(F32), nin_ref[0], nin_ref[1])
        gate_ref[i] = sigmoid(dot_nn(w_ref[...], zn) + b_ref[...])
        return carry
    lax.fori_loop(0, z_ref.shape[0], body, 0, unroll=4)


def gate_call(z_t, norm_in, w_gate, b_gate):
    n_i, n_z, cols = z_t.shape
    row_spec = pl.BlockSpec((n_i, n_z, J_BLK), lambda j: (0, 0, j))
    return pl.pallas_call(
        gate_kernel, grid=(cols // J_BLK,),
        in_specs=[row_spec, pl.BlockSpec(norm_in.shape, lambda j: (0, 0, 0)), pl.BlockSpec(w_gate.shape, lambda j: (0, 0)),
                  pl.BlockSpec(b_gate.shape, lambda j: (0, 0))],
        out_specs=row_spec, out_shape=jax.ShapeDtypeStruct(z_t.shape, F32),
        compiler_params=pltpu.CompilerParams(dimension_semantics=('arbitrary',)),
        cost_estimate=pl.CostEstimate(flops=12 * n_i * cols * n_z * n_z, bytes_accessed=6 * n_i * cols * n_z,
                                      transcendentals=n_i * cols * n_z),
        name='tri_gate',
    )(z_t, norm_in, w_gate, b_gate)


def emit_ab(ab_ref, s_refs):
    n_dev, _, n_cl, n_i, lanes = ab_ref.shape

    def body(dev, carry):
        for q in range(2):
            for c in range(n_cl):
                base = pl.multiple_of((dev * n_cl + c) * I_STRIDE, 8)
                for t in range(lanes // LANES):
                    ab_ref[dev, q, c, :, t * LANES:(t + 1) * LANES] = s_refs[q][t, pl.ds(base, n_i), :].astype(BF16)
        return carry
    lax.fori_loop(0, n_dev, body, 0, unroll=2)


def start_kernel(z_ref, u_ref, mask_ref, nin_ref, w_ref, b_ref, z_out, ab_ref, s_a, s_b):
    n_i = z_ref.shape[0]

    def body(i, carry):
        z_new = (z_ref[i].astype(F32) + u_ref[i].astype(F32)).astype(BF16)
        z_out[i] = z_new
        project_row(i, z_new.astype(F32), mask_ref[pl.ds(i, 1), :], nin_ref, w_ref, b_ref, (s_a, s_b))
        return carry
    lax.fori_loop(0, n_i, body, 0, unroll=ROW_UNROLL)
    emit_ab(ab_ref, (s_a, s_b))


def finish_stats(o_ref, s_o, r_ref):
    n_c, n_i, lanes = o_ref.shape
    total = lax.fori_loop(0, n_c, lambda c, acc: acc + o_ref[c], jnp.zeros((n_i, lanes), F32), unroll=16)
    mean_val = total / n_c

    def body(c, acc):
        base = pl.multiple_of(c * I_STRIDE, 8)
        centered = o_ref[c] - mean_val
        for t in range(lanes // LANES):
            s_o[t, pl.ds(base, n_i), :] = centered[:, t * LANES:(t + 1) * LANES]
        return acc + centered * centered
    square = lax.fori_loop(0, n_c, body, jnp.zeros((n_i, lanes), F32), unroll=16)
    r_ref[...] = lax.rsqrt(square / n_c + LN_EPS)


def finish_row(i, z_ref, gate_ref, nout_ref, wo_ref, bo_ref, s_o, r_ref):
    tiles, rows, _ = s_o.shape
    n_c = rows // I_STRIDE
    centered = jnp.concatenate([s_o[t, pl.ds(i, n_c, stride=I_STRIDE), :] for t in range(tiles)], axis=1)
    norm = (centered * r_ref[pl.ds(i, 1), :] * nout_ref[0] + nout_ref[1]).astype(BF16)
    upd = (dot_nn(wo_ref[...], norm) + bo_ref[...]).astype(BF16)
    return (z_ref[i].astype(F32) + gate_ref[i] * upd.astype(F32)).astype(BF16)


def middle_kernel(o_ref, zin_ref, gin_ref, nout_ref, wo_ref, bo_ref, u_ref, mask_ref, nin_ref, w_ref, b_ref,
                  z_out, ab_ref, s_a, s_b, s_o, r_ref):
    n_i = zin_ref.shape[0]
    finish_stats(o_ref, s_o, r_ref)

    def body(i, carry):
        z_mid = finish_row(i, zin_ref, gin_ref, nout_ref, wo_ref, bo_ref, s_o, r_ref)
        z_new = (z_mid.astype(F32) + u_ref[i].astype(F32)).astype(BF16)
        z_out[i] = z_new
        project_row(i, z_new.astype(F32), mask_ref[pl.ds(i, 1), :], nin_ref, w_ref, b_ref, (s_a, s_b))
        return carry
    lax.fori_loop(0, n_i, body, 0, unroll=ROW_UNROLL)
    emit_ab(ab_ref, (s_a, s_b))


def end_kernel(o_ref, zin_ref, gin_ref, nout_ref, wo_ref, bo_ref, z_out, s_o, r_ref):
    n_i = zin_ref.shape[0]
    finish_stats(o_ref, s_o, r_ref)

    def body(i, carry):
        z_new = finish_row(i, zin_ref, gin_ref, nout_ref, wo_ref, bo_ref, s_o, r_ref)
        z_out[i] = z_new.astype(F32).T.astype(BF16)
        return carry
    lax.fori_loop(0, n_i, body, 0, unroll=ROW_UNROLL)


J_BLK = 256


def tri_call(kind, n_dev, args):
    kernels = {'start': start_kernel, 'middle': middle_kernel, 'end': end_kernel}
    if kind == 'start':
        n_i, n_z, cols = args[0].shape
    else:
        n_i, n_z, cols = args[1].shape
    n_ch = n_z

    def blk(arr, which):
        shape = arr.shape
        if which == 'j':
            return pl.BlockSpec(shape[:-1] + (J_BLK,), lambda j: (0,) * (len(shape) - 1) + (j,))
        return pl.BlockSpec(shape, lambda j: (0,) * len(shape))

    tiles = J_BLK // LANES
    fin = ['j', 'j', 'j', 'w', 'w', 'w']
    pro = ['j', 'j', 'w', 'w', 'w']
    kinds = {'start': ['j'] + pro, 'middle': fin + pro, 'end': fin}[kind]
    scr = pltpu.VMEM((tiles, n_ch * I_STRIDE, LANES), F32)
    stat = pltpu.VMEM((n_i, J_BLK), F32)
    if kind == 'end':
        out_shape = jax.ShapeDtypeStruct((n_i, cols, n_z), BF16)
        out_specs = pl.BlockSpec((n_i, J_BLK, n_z), lambda j: (0, j, 0))
        scratch = [scr, stat]
    else:
        out_shape = (jax.ShapeDtypeStruct((n_i, n_z, cols), BF16),
                     jax.ShapeDtypeStruct((n_dev, 2, n_ch // n_dev, n_i, cols), BF16))
        out_specs = tuple(blk(s, 'j') for s in out_shape)
        scratch = [scr, scr] + ([scr, stat] if kind == 'middle' else [])
    return pl.pallas_call(
        kernels[kind], grid=(cols // J_BLK,),
        in_specs=[blk(a, k) for a, k in zip(args, kinds)],
        out_specs=out_specs, out_shape=out_shape, scratch_shapes=scratch,
        compiler_params=pltpu.CompilerParams(dimension_semantics=('arbitrary',)),
        cost_estimate=pl.CostEstimate(flops=12 * n_i * cols * n_z * n_z, bytes_accessed=16 * n_i * cols * n_z,
                                      transcendentals=3 * n_i * cols * n_z),
        name='tri_' + kind,
    )(*args)


def product_kernel(ab_ref, o_ref):
    n_dev, _, _, n_i, cols = ab_ref.shape
    left = ab_ref[:, 0, 0].reshape(n_dev * n_i, cols)
    right = ab_ref[:, 1, 0].reshape(n_dev * n_i, cols)
    half = cols // 2
    for h in range(2):
        o_ref[:, 0, :, h * half:(h + 1) * half] = dot_nt(left, right[h * half:(h + 1) * half]).reshape(n_dev, n_i, half)


def tri_product(ab):
    n_dev, _, n_cl, n_i, cols = ab.shape
    rows = n_dev * n_i
    return pl.pallas_call(
        product_kernel, grid=(n_cl,),
        in_specs=[pl.BlockSpec((n_dev, 2, 1, n_i, cols), lambda c: (0, 0, c, 0, 0))],
        out_specs=pl.BlockSpec((n_dev, 1, n_i, cols), lambda c: (0, c, 0, 0)),
        out_shape=jax.ShapeDtypeStruct((n_dev, n_cl, n_i, cols), F32),
        compiler_params=pltpu.CompilerParams(dimension_semantics=('arbitrary',)),
        cost_estimate=pl.CostEstimate(flops=2 * n_cl * rows * rows * cols, bytes_accessed=8 * n_cl * rows * cols,
                                      transcendentals=0),
        name='tri_product',
    )(ab)


def solution(mesh):
    pair_spec = P(('batch', 'dap'), None, None)
    mask_spec = P(('batch', 'dap'), None)
    msa_spec = P(None, ('batch', 'dap'), None)
    n_dev = mesh.shape['dap']

    def column(vec):
        return vec.astype(F32)[..., None]

    def device_fn(pair_act, pair_mask, msa_act, opm_norm, opm_w_in, opm_b_in, opm_w_out, opm_b_out, tri_norm_in, tri_w_ab, tri_b_ab, tri_w_gate, tri_b_gate, tri_norm_out, tri_w_out, tri_b_out):
        layers = opm_norm.shape[0]
        n_i, cols, n_z = pair_act.shape
        n_c = opm_w_in.shape[-1]
        mask_f = pair_mask.astype(F32)
        n_m = msa_act.shape[-1]
        w_bd = jnp.zeros((layers, n_m, layers, 2 * n_c), BF16)
        for l in range(layers):
            w_bd = w_bd.at[l, :, l].set(opm_w_in[l].reshape(n_m, 2 * n_c))
        sides = msa_project(msa_act, opm_norm.astype(F32), w_bd.reshape(layers * n_m, layers * 2 * n_c),
                                  opm_b_in.astype(F32).reshape(1, -1))
        left, right = sides[:layers], sides[layers:]
        opm_w = [opm_w_out[l].reshape(n_c, n_c, n_z).transpose(2, 1, 0).reshape(n_z, n_c * n_c) for l in range(layers)]
        gathered = ring_gather(right[0], n_dev, 'dap', 0)
        updates = []
        for l in range(layers):
            rest = (left[l], gathered, opm_w[l], column(opm_b_out[l]))
            if l + 1 < layers:
                gathered, update = gather_with_opm(right[l + 1], n_dev, 'dap', l + 1, *rest)
            else:
                update = opm_update(*rest)
            updates.append(update)
        z_t = jnp.swapaxes(pair_act, 1, 2)
        fin = None
        for l in range(layers):
            w_all = tri_w_ab[l].transpose(1, 2, 0).reshape(-1, n_z)
            norm_in = column(tri_norm_in[l])
            pro = (updates[l], mask_f, norm_in, w_all, column(tri_b_ab[l].reshape(-1)))
            if l == 0:
                z_t, ab = tri_call('start', n_dev, (z_t,) + pro)
            else:
                z_t, ab = tri_call('middle', n_dev, fin + pro)
            ab = lax.all_to_all(ab.reshape(n_dev, -1, cols), 'dap', 0, 0, tiled=True).reshape(ab.shape)
            prod, z_g = lax.optimization_barrier((tri_product(ab), z_t))
            gate = gate_call(z_g, norm_in, tri_w_gate[l].T, column(tri_b_gate[l]))
            prod = lax.all_to_all(prod, 'dap', 0, 0, tiled=True)
            fin = (prod.reshape(-1, n_i, cols), z_t, gate, column(tri_norm_out[l]), tri_w_out[l].T, column(tri_b_out[l]))
        return tri_call('end', n_dev, fin)

    return jax.shard_map(device_fn, mesh=mesh, in_specs=(pair_spec, mask_spec, msa_spec) + (P(),) * 13, out_specs=pair_spec, check_vma=False)
```

```python
import functools
import math
import jax
import jax.numpy as jnp
from jax import lax
from jax.experimental import pallas as pl
from jax.experimental.pallas import tpu as pltpu
from jax.sharding import PartitionSpec as P

LN_EPS = 1e-5
LANES = 128
ROW_UNROLL = 8
F32 = jnp.float32
BF16 = jnp.bfloat16


COLUMN_PARTS = 11
OPM_BIAS, NORM_IN, PROJ_BIAS, GATE_BIAS, NORM_OUT, OUT_BIAS = 0, 1, 3, 7, 8, 10


def col(ref, part, count=1):
    size = ref.shape[0] // COLUMN_PARTS
    return ref[part * size:(part + count) * size]


def pack_columns(parts):
    total, offset, out = sum(p.shape[0] for p in parts), 0, 0.0
    for p in parts:
        out = out + lax.pad(p.astype(F32), jnp.float32(0), [(offset, total - offset - p.shape[0], 0)])
        offset += p.shape[0]
    return out[:, None]


def dot_nn(a, b):
    return lax.dot_general(a, b, (((1,), (0,)), ((), ())), preferred_element_type=F32)


def dot_nt(a, b):
    return lax.dot_general(a, b, (((1,), (1,)), ((), ())), preferred_element_type=F32)


I_STRIDE = 24
S_GROUP = 32


def msa_kernel(m_ref, norm_ref, w_ref, bias_ref, *refs):
    y_ref, t_ref = refs[-2:]
    layers = t_ref.shape[0]
    a_refs, b_refs = refs[:layers], refs[layers:2 * layers]
    s_blk, n_i, _ = m_ref.shape
    n_c = b_refs[0].shape[0]
    group = S_GROUP
    gains = [norm_ref[l].astype(F32) for l in range(layers)]

    def rows(g, carry):
        base = pl.multiple_of(g * group, group)
        x = m_ref[pl.ds(base, group)].astype(F32).reshape(group * n_i, -1)
        mean_val = jnp.mean(x, axis=-1, keepdims=True)
        centered = x - mean_val
        var_val = jnp.mean(centered * centered, axis=-1, keepdims=True)
        scaled = centered * lax.rsqrt(var_val + LN_EPS)
        normed = jnp.concatenate([(scaled * gains[l][0:1] + gains[l][1:2]).astype(BF16) for l in range(layers)], axis=1)
        proj = dot_nn(normed, w_ref[...]) + bias_ref[...]
        for s in range(group):
            y_ref[pl.ds(pl.multiple_of((base + s) * I_STRIDE, 8), n_i), :] = proj[s * n_i:(s + 1) * n_i]
        return carry
    lax.fori_loop(0, s_blk // group, rows, 0, unroll=2)

    def columns(i, carry):
        flip = y_ref[pl.ds(i, s_blk, stride=I_STRIDE), :].T
        for l in range(layers):
            top = 2 * l * n_c
            a_refs[l][pl.ds(pl.multiple_of(i * n_c, n_c), n_c), :] = flip[top:top + n_c].astype(BF16)
            t_ref[l, pl.ds(i, n_c, stride=I_STRIDE), :] = flip[top + n_c:top + 2 * n_c]
        return carry
    lax.fori_loop(0, n_i, columns, 0, unroll=4)
    for l in range(layers):
        for d in range(n_c):
            b_refs[l][d] = t_ref[l, d * I_STRIDE:d * I_STRIDE + n_i, :].astype(BF16)


def msa_project(msa_act, norm_w, w_bd, bias):
    seqs, n_i, n_m = msa_act.shape
    layers = norm_w.shape[0]
    n_c = w_bd.shape[1] // (2 * layers)
    s_blk = LANES
    return pl.pallas_call(
        msa_kernel, grid=(seqs // s_blk,),
        in_specs=[
            pl.BlockSpec((s_blk, n_i, n_m), lambda s: (s, 0, 0)),
            pl.BlockSpec(norm_w.shape, lambda s: (0, 0, 0)),
            pl.BlockSpec(w_bd.shape, lambda s: (0, 0)),
            pl.BlockSpec(bias.shape, lambda s: (0, 0)),
        ],
        out_specs=(pl.BlockSpec((n_i * n_c, s_blk), lambda s: (0, s)),) * layers
        + (pl.BlockSpec((n_c, n_i, s_blk), lambda s: (0, 0, s)),) * layers,
        out_shape=(jax.ShapeDtypeStruct((n_i * n_c, seqs), BF16),) * layers
        + (jax.ShapeDtypeStruct((n_c, n_i, seqs), BF16),) * layers,
        scratch_shapes=[pltpu.VMEM((s_blk * I_STRIDE, w_bd.shape[1]), F32),
                        pltpu.VMEM((layers, n_c * I_STRIDE, s_blk), F32)],
        compiler_params=pltpu.CompilerParams(dimension_semantics=('arbitrary',)),
        cost_estimate=pl.CostEstimate(flops=2 * seqs * n_i * n_m * 2 * n_c * layers,
                                      bytes_accessed=2 * seqs * n_i * (n_m + 2 * n_c * layers), transcendentals=0),
        name='msa_project',
    )(msa_act, norm_w, w_bd, bias)


def opm_kernel(inv_s, first, last, a_ref, b_ref, w_ref, bias_ref, *rest):
    acc_ref, out_ref, q_ref = (None,) * first + rest
    part = pl.program_id(1)
    dev, d_blk, j_loc, seqs = b_ref.shape
    n_i, _, j_blk = q_ref.shape
    n_c = a_ref.shape[0] // n_i
    for d in range(d_blk):
        rhs = b_ref[:, d, :, :].reshape(dev * j_loc, seqs)
        prod = (dot_nt(a_ref[...], rhs) * inv_s).astype(BF16)
        base = pl.multiple_of((part * d_blk + d) * n_c, n_c)
        q_ref[:, pl.ds(base, n_c), :] = prod.reshape(n_i, n_c, j_blk)

    @pl.when(part == pl.num_programs(1) - 1)
    def _():
        def body(i, carry):
            upd = dot_nn(w_ref[...], q_ref[i])
            if not first:
                upd = acc_ref[i] + upd
            out_ref[i] = (upd + col(bias_ref, OPM_BIAS)).astype(BF16) if last else upd
            return carry
        lax.fori_loop(0, n_i, body, 0, unroll=4)


def opm_update(a_t, b_all, w_t, bias, acc=None, last=True):
    n_dev, n_d, j_loc, seqs = b_all.shape
    rows_c = a_t.shape[0]
    n_z = w_t.shape[0]
    n_c = w_t.shape[1] // n_d
    n_i = rows_c // n_c
    cols = n_dev * j_loc
    j_blk = 2 * LANES
    dev_blk = j_blk // j_loc
    d_blk = math.gcd(n_d, 8)
    grid = (cols // j_blk, n_d // d_blk)
    row_spec = pl.BlockSpec((n_i, n_z, j_blk), lambda j, d: (0, 0, j))
    first = acc is None
    return pl.pallas_call(
        functools.partial(opm_kernel, 1.0 / seqs, first, last),
        grid=grid,
        in_specs=[
            pl.BlockSpec((rows_c, seqs), lambda j, d: (0, 0)),
            pl.BlockSpec((dev_blk, d_blk, j_loc, seqs), lambda j, d: (j, d, 0, 0)),
            pl.BlockSpec(w_t.shape, lambda j, d: (0, 0)),
            pl.BlockSpec(bias.shape, lambda j, d: (0, 0)),
        ] + ([] if first else [row_spec]),
        out_specs=row_spec,
        out_shape=jax.ShapeDtypeStruct((n_i, n_z, cols), BF16 if last else F32),
        scratch_shapes=[pltpu.VMEM((n_i, n_d * n_c, j_blk), BF16)],
        compiler_params=pltpu.CompilerParams(dimension_semantics=('arbitrary', 'arbitrary')),
        cost_estimate=pl.CostEstimate(
            flops=2 * rows_c * seqs * cols * n_d + 2 * n_i * cols * n_d * n_c * n_z,
            bytes_accessed=2 * (n_dev * n_d * j_loc * seqs + n_i * n_z * cols), transcendentals=0),
        name='opm_update',
    )(a_t, b_all, w_t, bias, *(() if first else (acc,)))


MESH_ID = pl.DeviceIdType.MESH
AG_UNITS = 4


class RingGather:
    def __init__(self, n, axis, src_ref, out_ref, r_sem, p_sem, s_sem, l_sem):
        self.n, self.side, self.axis = n, math.isqrt(n // 2), axis
        self.src, self.out = src_ref, out_ref
        self.r_sem, self.p_sem, self.s_sem, self.l_sem = r_sem, p_sem, s_sem, l_sem
        me = lax.axis_index(axis)
        self.me, self.core = me, me % 2
        self.x, self.y = (me // 2) % self.side, me // (2 * self.side)
        self.size = src_ref.shape[0] // AG_UNITS

    def at(self, u, k1, k2, other=False):
        kx, ky = (k1, k2) if u < AG_UNITS // 2 else (k2, k1)
        core = 1 - self.core if other else self.core
        return (((self.y + ky) % self.side) * self.side + (self.x + kx) % self.side) * 2 + core

    def neighbours(self):
        last = self.side - 1
        return [self.at(0, 1, 0), self.at(0, last, 0), self.at(0, 0, 1), self.at(0, 0, last), self.at(0, 0, 0, True)]

    def barrier(self):
        sem = pltpu.get_barrier_semaphore()
        peers = self.neighbours()
        for p in peers:
            pl.semaphore_signal(sem, inc=1, device_id={self.axis: p}, device_id_type=MESH_ID)
        pl.semaphore_wait(sem, len(peers))

    def copy(self, u, k1, k2, way):
        rows = pl.ds(u * self.size, self.size)
        owner = self.at(u, k1, k2)
        src = self.src.at[rows] if (k1, k2) == (0, 0) else self.out.at[owner, rows]
        step = (1, self.side - 1)[way % 2]
        if way < 2:
            dest, rk, sems = self.at(u, step, 0), ((k1 - step) % self.side, k2), self.r_sem
        elif way < 4:
            dest, rk, sems = self.at(u, 0, step), (k1, (k2 - step) % self.side), self.r_sem
        else:
            dest, rk, sems = self.at(u, 0, 0, True), (k1, k2), self.p_sem
        return pltpu.make_async_remote_copy(src, self.out.at[owner, rows], self.s_sem.at[u, k1, k2, way], sems.at[u, rk[0], rk[1]],
                                            device_id={self.axis: dest}, device_id_type=MESH_ID)

    def ways(self, u, k1, k2):
        last = self.side - 1
        plus = u % 2 == 0
        out = []
        if k2 == 0:
            if k1 == 0:
                out += [0, 1]
            elif k1 == last and plus:
                out.append(0)
            elif k1 == 1 and not plus:
                out.append(1)
            out += [2, 3]
        elif k2 == last and plus:
            out.append(2)
        elif k2 == 1 and not plus:
            out.append(3)
        return out + [4]

    def arrived(self, u, k1, k2, sems, other=False):
        rows = pl.ds(u * self.size, self.size)
        dst = self.out.at[self.at(u, k1, k2, other), rows]
        pltpu.make_async_remote_copy(dst, dst, self.s_sem.at[u, k1, k2, 4], sems.at[u, k1, k2],
                                     device_id={self.axis: self.at(0, 0, 0, True)}, device_id_type=MESH_ID).wait_recv()

    def steps(self):
        last = self.side - 1
        units = range(AG_UNITS)
        own = pltpu.make_async_copy(self.src, self.out.at[self.me], self.l_sem)

        def begin():
            own.start()
            for pair in ((0, 1), (2, 3), (4,)):
                for u in units:
                    for way in pair:
                        self.copy(u, 0, 0, way).start()

        def relay(k1, k2):
            for u in units:
                self.arrived(u, k1, k2, self.r_sem)
                for way in self.ways(u, k1, k2):
                    self.copy(u, k1, k2, way).start()

        def finish():
            for k1 in range(self.side):
                for k2 in range(self.side):
                    for u in units:
                        self.arrived(u, k1, k2, self.p_sem, True)
            for k1 in range(self.side):
                for k2 in range(self.side):
                    for u in units:
                        for way in self.ways(u, k1, k2):
                            self.copy(u, k1, k2, way).wait_send()
            own.wait()
        order = [(last, 0), (1, 0), (0, last), (0, 1), (2, 0)]
        order += [(k1, k2) for k1 in (last, 1, 2) for k2 in (last, 1)]
        order += [(k1, 2) for k1 in (0, last, 1, 2)]
        return [begin] + [functools.partial(relay, *o) for o in order] + [finish]


def gather_kernel(n, axis, src_ref, out_ref, *sems):
    ring = RingGather(n, axis, src_ref, out_ref, *sems)
    ring.barrier()
    for step in ring.steps():
        step()


def gather_scratch(side):
    dma = pltpu.SemaphoreType.DMA
    return [dma((AG_UNITS, side, side)), dma((AG_UNITS, side, side)), dma((AG_UNITS, side, side, 5)), dma]


def ring_gather(block, n, axis, cid):
    side = math.isqrt(n // 2)
    assert 2 * side * side == n and side == 4
    return pl.pallas_call(
        functools.partial(gather_kernel, n, axis),
        out_shape=jax.ShapeDtypeStruct((n,) + block.shape, block.dtype),
        in_specs=[pl.BlockSpec(memory_space=pl.ANY)], out_specs=pl.BlockSpec(memory_space=pl.ANY),
        scratch_shapes=gather_scratch(side),
        compiler_params=pltpu.CompilerParams(collective_id=cid, has_side_effects=True),
        name='ring_gather',
    )(block)


def gather_opm_kernel(n, axis, inv_s, src_ref, a_ref, b_ref, w_ref, c_ref, z_ref, mask_ref, w_ab_ref, out_ref, z_out, ab_ref,
                      buf, q_ref, upd_ref, s_a, s_b, b_sem, *sems):
    ring = RingGather(n, axis, src_ref, out_ref, *sems)
    _, dev_blk, d_blk, j_loc, seqs = buf.shape
    n_i, _, j_blk = q_ref.shape
    n_c = a_ref.shape[0] // n_i
    parts = b_ref.shape[1] // d_blk
    total = (b_ref.shape[0] // dev_blk) * parts

    def load(k):
        j, part = k // parts, k % parts
        return pltpu.make_async_copy(b_ref.at[pl.ds(j * dev_blk, dev_blk), pl.ds(part * d_blk, d_blk)], buf.at[k % 2], b_sem.at[k % 2])

    def outer(k):
        if k + 1 < total:
            load(k + 1).start()
        load(k).wait()

        def body(d, carry):
            rhs = buf[k % 2, :, d].reshape(dev_blk * j_loc, seqs)
            prod = (dot_nt(a_ref[...], rhs) * inv_s).astype(BF16)
            base = pl.multiple_of(((k % parts) * d_blk + d) * n_c, n_c)
            q_ref[:, pl.ds(base, n_c), :] = prod.reshape(n_i, n_c, j_blk)
            return carry
        lax.fori_loop(0, d_blk, body, 0, unroll=2)

    def contract(j, low, high):
        def body(i, carry):
            upd = dot_nn(w_ref[...], q_ref[i]) + col(c_ref, OPM_BIAS)
            upd_ref[i, :, j * j_blk:(j + 1) * j_blk] = upd.astype(BF16)
            return carry
        lax.fori_loop(low, high, body, 0, unroll=4)
    pieces = []
    for k in range(total):
        pieces.append(functools.partial(outer, k))
        if k % parts == parts - 1:
            for half in range(2):
                pieces.append(functools.partial(contract, k // parts, half * n_i // 2, (half + 1) * n_i // 2))

    def project(j, low, high):
        lanes = slice(j * j_blk, (j + 1) * j_blk)

        def body(i, carry):
            z_old = z_ref[i, lanes, :].astype(F32).T
            z_new = (z_old + upd_ref[i, :, lanes].astype(F32)).astype(BF16)
            z_out[i, :, lanes] = z_new
            project_row(i, z_new.astype(F32), mask_ref[pl.ds(i, 1), lanes].astype(F32), w_ab_ref, c_ref, (s_a, s_b),
                        j * j_blk // LANES)
            return carry
        lax.fori_loop(low, high, body, 0, unroll=2)
    for j in range(total // parts):
        for quarter in range(4):
            pieces.append(functools.partial(project, j, quarter * n_i // 4, (quarter + 1) * n_i // 4))
    n_dest = ab_ref.shape[0]
    for half in range(2):
        pieces.append(functools.partial(emit_ab, ab_ref, (s_a, s_b), half * n_dest // 2, (half + 1) * n_dest // 2))
    load(0).start()
    ring.barrier()
    steps = ring.steps()
    done = 0
    for k, step in enumerate(steps[:-1]):
        step()
        while done * (len(steps) - 1) < (k + 1) * len(pieces):
            pieces[done]()
            done += 1
    steps[-1]()


def gather_with_opm(block, n, axis, cid, a_t, b_all, w_t, cols_l, pair_act, pair_mask, w_ab):
    n_dev, n_d, j_loc, seqs = b_all.shape
    n_z = w_t.shape[0]
    n_c = w_t.shape[1] // n_d
    n_i = a_t.shape[0] // n_c
    cols = n_dev * j_loc
    j_blk = 2 * LANES
    d_blk = math.gcd(n_d, 8)
    side = math.isqrt(n // 2)
    assert 2 * side * side == n and side == 4
    ab_scr = pltpu.VMEM((cols // LANES, n_z * I_STRIDE, LANES), F32)
    any_spec = pl.BlockSpec(memory_space=pl.ANY)
    vmem_spec = pl.BlockSpec(memory_space=pltpu.VMEM)
    return pl.pallas_call(
        functools.partial(gather_opm_kernel, n, axis, 1.0 / seqs),
        out_shape=(jax.ShapeDtypeStruct((n,) + block.shape, block.dtype), jax.ShapeDtypeStruct((n_i, n_z, cols), BF16),
                   jax.ShapeDtypeStruct((n, 2, n_z // n, n_i, cols), BF16)),
        in_specs=[any_spec, vmem_spec, any_spec] + [vmem_spec] * 5, out_specs=(any_spec, vmem_spec, vmem_spec),
        scratch_shapes=[pltpu.VMEM((2, j_blk // j_loc, d_blk, j_loc, seqs), BF16), pltpu.VMEM((n_i, n_d * n_c, j_blk), BF16),
                        pltpu.VMEM((n_i, n_z, cols), BF16), ab_scr, ab_scr, pltpu.SemaphoreType.DMA((2,))] + gather_scratch(side),
        compiler_params=pltpu.CompilerParams(collective_id=cid, has_side_effects=True),
        cost_estimate=pl.CostEstimate(flops=2 * a_t.shape[0] * seqs * cols * n_d * 4, bytes_accessed=2 * b_all.size, transcendentals=0),
        name='ring_gather_opm',
    )(block, a_t, b_all, w_t, cols_l, pair_act, pair_mask, w_ab)


def norm_columns(x_f32, gain, offset):
    mean_val = jnp.mean(x_f32, axis=0, keepdims=True)
    centered = x_f32 - mean_val
    var_val = jnp.mean(centered * centered, axis=0, keepdims=True)
    return (centered * lax.rsqrt(var_val + LN_EPS) * gain + offset).astype(BF16)


def sigmoid(x):
    return 0.5 * jnp.tanh(0.5 * x) + 0.5


def project_row(i, z_f32, mask_row, w_ref, c_ref, s_refs, tile0=0):
    zn = norm_columns(z_f32, col(c_ref, NORM_IN), col(c_ref, NORM_IN + 1))
    n_z, lanes = z_f32.shape
    n_ch = w_ref.shape[0] // 4
    proj = dot_nn(w_ref[...], zn) + col(c_ref, PROJ_BIAS, 4)
    for q in range(2):
        lin = proj[2 * q * n_ch:(2 * q + 1) * n_ch]
        sig = sigmoid(proj[(2 * q + 1) * n_ch:(2 * q + 2) * n_ch])
        val = mask_row * sig * lin
        for t in range(lanes // LANES):
            s_refs[q][tile0 + t, pl.ds(i, n_ch, stride=I_STRIDE), :] = val[:, t * LANES:(t + 1) * LANES]


def gate_kernel(z_ref, w_ref, c_ref, gate_ref):
    def body(i, carry):
        zn = norm_columns(z_ref[i].astype(F32), col(c_ref, NORM_IN), col(c_ref, NORM_IN + 1))
        gate_ref[i] = sigmoid(dot_nn(w_ref[...], zn) + col(c_ref, GATE_BIAS))
        return carry
    lax.fori_loop(0, z_ref.shape[0], body, 0, unroll=4)


def gate_call(z_t, w_gate, cols_l):
    n_i, n_z, cols = z_t.shape
    row_spec = pl.BlockSpec((n_i, n_z, J_BLK), lambda j: (0, 0, j))
    return pl.pallas_call(
        gate_kernel, grid=(cols // J_BLK,),
        in_specs=[row_spec, pl.BlockSpec(w_gate.shape, lambda j: (0, 0)), pl.BlockSpec(cols_l.shape, lambda j: (0, 0))],
        out_specs=row_spec, out_shape=jax.ShapeDtypeStruct(z_t.shape, F32),
        compiler_params=pltpu.CompilerParams(dimension_semantics=('arbitrary',)),
        cost_estimate=pl.CostEstimate(flops=12 * n_i * cols * n_z * n_z, bytes_accessed=6 * n_i * cols * n_z,
                                      transcendentals=n_i * cols * n_z),
        name='tri_gate',
    )(z_t, w_gate, cols_l)


def emit_ab(ab_ref, s_refs, low=0, high=None):
    n_dev, _, n_cl, n_i, lanes = ab_ref.shape
    high = n_dev if high is None else high

    def body(dev, carry):
        for q in range(2):
            for c in range(n_cl):
                base = pl.multiple_of((dev * n_cl + c) * I_STRIDE, 8)
                for t in range(lanes // LANES):
                    ab_ref[dev, q, c, :, t * LANES:(t + 1) * LANES] = s_refs[q][t, pl.ds(base, n_i), :].astype(BF16)
        return carry
    lax.fori_loop(low, high, body, 0, unroll=2)


def finish_stats(o_ref, s_o, r_ref):
    n_c, n_i, lanes = o_ref.shape
    total = lax.fori_loop(0, n_c, lambda c, acc: acc + o_ref[c], jnp.zeros((n_i, lanes), F32), unroll=16)
    mean_val = total / n_c

    def body(c, acc):
        base = pl.multiple_of(c * I_STRIDE, 8)
        centered = o_ref[c] - mean_val
        for t in range(lanes // LANES):
            s_o[t, pl.ds(base, n_i), :] = centered[:, t * LANES:(t + 1) * LANES]
        return acc + centered * centered
    square = lax.fori_loop(0, n_c, body, jnp.zeros((n_i, lanes), F32), unroll=16)
    r_ref[...] = lax.rsqrt(square / n_c + LN_EPS)


def finish_row(i, z_ref, gate_ref, wo_ref, c_ref, s_o, r_ref):
    tiles, rows, _ = s_o.shape
    n_c = rows // I_STRIDE
    centered = jnp.concatenate([s_o[t, pl.ds(i, n_c, stride=I_STRIDE), :] for t in range(tiles)], axis=1)
    norm = (centered * r_ref[pl.ds(i, 1), :] * col(c_ref, NORM_OUT) + col(c_ref, NORM_OUT + 1)).astype(BF16)
    upd = (dot_nn(wo_ref[...], norm) + col(c_ref, OUT_BIAS)).astype(BF16)
    return (z_ref[i].astype(F32) + gate_ref[i] * upd.astype(F32)).astype(BF16)


def middle_kernel(o_ref, zin_ref, gin_ref, wo_ref, cp_ref, u_ref, mask_ref, w_ref, c_ref,
                  z_out, ab_ref, s_a, s_b, s_o, r_ref):
    n_i = zin_ref.shape[0]
    finish_stats(o_ref, s_o, r_ref)

    def body(i, carry):
        z_mid = finish_row(i, zin_ref, gin_ref, wo_ref, cp_ref, s_o, r_ref)
        z_new = (z_mid.astype(F32) + u_ref[i].astype(F32)).astype(BF16)
        z_out[i] = z_new
        project_row(i, z_new.astype(F32), mask_ref[pl.ds(i, 1), :].astype(F32), w_ref, c_ref, (s_a, s_b))
        return carry
    lax.fori_loop(0, n_i, body, 0, unroll=ROW_UNROLL)
    emit_ab(ab_ref, (s_a, s_b))


def end_kernel(o_ref, zin_ref, gin_ref, wo_ref, c_ref, z_out, s_o, r_ref):
    n_i = zin_ref.shape[0]
    finish_stats(o_ref, s_o, r_ref)

    def body(i, carry):
        z_new = finish_row(i, zin_ref, gin_ref, wo_ref, c_ref, s_o, r_ref)
        z_out[i] = z_new.astype(F32).T.astype(BF16)
        return carry
    lax.fori_loop(0, n_i, body, 0, unroll=ROW_UNROLL)


J_BLK = 256


def tri_call(kind, n_dev, args):
    kernels = {'middle': middle_kernel, 'end': end_kernel}
    n_i, n_z, cols = args[1].shape
    n_ch = n_z

    def blk(arr, which):
        shape = arr.shape
        if which == 'j':
            return pl.BlockSpec(shape[:-1] + (J_BLK,), lambda j: (0,) * (len(shape) - 1) + (j,))
        return pl.BlockSpec(shape, lambda j: (0,) * len(shape))

    tiles = J_BLK // LANES
    fin = ['j', 'j', 'j', 'w', 'w']
    kinds = {'middle': fin + ['j', 'j', 'w', 'w'], 'end': fin}[kind]
    scr = pltpu.VMEM((tiles, n_ch * I_STRIDE, LANES), F32)
    stat = pltpu.VMEM((n_i, J_BLK), F32)
    if kind == 'end':
        out_shape = jax.ShapeDtypeStruct((n_i, cols, n_z), BF16)
        out_specs = pl.BlockSpec((n_i, J_BLK, n_z), lambda j: (0, j, 0))
        scratch = [scr, stat]
    else:
        out_shape = (jax.ShapeDtypeStruct((n_i, n_z, cols), BF16),
                     jax.ShapeDtypeStruct((n_dev, 2, n_ch // n_dev, n_i, cols), BF16))
        out_specs = tuple(blk(s, 'j') for s in out_shape)
        scratch = [scr, scr] + ([scr, stat] if kind == 'middle' else [])
    return pl.pallas_call(
        kernels[kind], grid=(cols // J_BLK,),
        in_specs=[blk(a, k) for a, k in zip(args, kinds)],
        out_specs=out_specs, out_shape=out_shape, scratch_shapes=scratch,
        compiler_params=pltpu.CompilerParams(dimension_semantics=('arbitrary',)),
        cost_estimate=pl.CostEstimate(flops=12 * n_i * cols * n_z * n_z, bytes_accessed=16 * n_i * cols * n_z,
                                      transcendentals=3 * n_i * cols * n_z),
        name='tri_' + kind,
    )(*args)


def product_kernel(ab_ref, o_ref):
    n_dev, _, _, n_i, cols = ab_ref.shape
    left = ab_ref[:, 0, 0].reshape(n_dev * n_i, cols)
    right = ab_ref[:, 1, 0].reshape(n_dev * n_i, cols)
    half = cols // 2
    for h in range(2):
        o_ref[:, 0, :, h * half:(h + 1) * half] = dot_nt(left, right[h * half:(h + 1) * half]).reshape(n_dev, n_i, half)


def tri_product(ab):
    n_dev, _, n_cl, n_i, cols = ab.shape
    rows = n_dev * n_i
    return pl.pallas_call(
        product_kernel, grid=(n_cl,),
        in_specs=[pl.BlockSpec((n_dev, 2, 1, n_i, cols), lambda c: (0, 0, c, 0, 0))],
        out_specs=pl.BlockSpec((n_dev, 1, n_i, cols), lambda c: (0, c, 0, 0)),
        out_shape=jax.ShapeDtypeStruct((n_dev, n_cl, n_i, cols), F32),
        compiler_params=pltpu.CompilerParams(dimension_semantics=('arbitrary',)),
        cost_estimate=pl.CostEstimate(flops=2 * n_cl * rows * rows * cols, bytes_accessed=8 * n_cl * rows * cols,
                                      transcendentals=0),
        name='tri_product',
    )(ab)


def solution(mesh):
    pair_spec = P(('batch', 'dap'), None, None)
    mask_spec = P(('batch', 'dap'), None)
    msa_spec = P(None, ('batch', 'dap'), None)
    n_dev = mesh.shape['dap']

    def device_fn(pair_act, pair_mask, msa_act, opm_norm, opm_w_in, opm_b_in, opm_w_out, opm_b_out, tri_norm_in, tri_w_ab, tri_b_ab, tri_w_gate, tri_b_gate, tri_norm_out, tri_w_out, tri_b_out):
        layers = opm_norm.shape[0]
        assert layers == 2
        n_i, cols, n_z = pair_act.shape
        n_c = opm_w_in.shape[-1]
        n_m = msa_act.shape[-1]
        same = jnp.arange(layers)[:, None] == jnp.arange(layers)[None, :]
        w_bd = jnp.where(same[:, None, :, None], opm_w_in.reshape(layers, n_m, 1, 2 * n_c), 0)
        sides = msa_project(msa_act, opm_norm, w_bd.reshape(layers * n_m, layers * 2 * n_c).astype(BF16),
                            opm_b_in.astype(F32).reshape(1, -1))
        left, right = sides[:layers], sides[layers:]
        opm_w = [opm_w_out[l].reshape(n_c, n_c, n_z).transpose(2, 1, 0).reshape(n_z, n_c * n_c) for l in range(layers)]
        w_abs = [tri_w_ab[l].transpose(1, 2, 0).reshape(-1, n_z) for l in range(layers)]
        params = [pack_columns([p[l].reshape(-1) for p in (opm_b_out, tri_norm_in, tri_b_ab, tri_b_gate, tri_norm_out, tri_b_out)])
                  for l in range(layers)]
        gathered = ring_gather(right[0], n_dev, 'dap', 0)
        gathered, z_t, ab = gather_with_opm(right[1], n_dev, 'dap', 1, left[0], gathered, opm_w[0], params[0], pair_act, pair_mask,
                                            w_abs[0])
        update = opm_update(left[1], gathered, opm_w[1], params[1])
        fin = None
        for l in range(layers):
            if l:
                z_t, ab = tri_call('middle', n_dev, fin + (update, pair_mask, w_abs[l], params[l]))
            ab = lax.all_to_all(ab.reshape(n_dev, -1, cols), 'dap', 0, 0, tiled=True).reshape(ab.shape)
            prod, z_g = lax.optimization_barrier((tri_product(ab), z_t))
            gate = gate_call(z_g, tri_w_gate[l].T, params[l])
            prod = lax.all_to_all(prod, 'dap', 0, 0, tiled=True)
            fin = (prod.reshape(-1, n_i, cols), z_t, gate, tri_w_out[l].T, params[l])
        return tri_call('end', n_dev, fin)

    return jax.shard_map(device_fn, mesh=mesh, in_specs=(pair_spec, mask_spec, msa_spec) + (P(),) * 13, out_specs=pair_spec, check_vma=False)
```

```python
import functools
import math
import jax
import jax.numpy as jnp
from jax import lax
from jax.experimental import pallas as pl
from jax.experimental.pallas import tpu as pltpu
from jax.sharding import PartitionSpec as P

LN_EPS = 1e-5
LANES = 128
ROW_UNROLL = 8
F32 = jnp.float32
BF16 = jnp.bfloat16


COLUMN_PARTS = 11
OPM_BIAS, NORM_IN, PROJ_BIAS, GATE_BIAS, NORM_OUT, OUT_BIAS = 0, 1, 3, 7, 8, 10


def col(ref, part, count=1):
    size = ref.shape[0] // COLUMN_PARTS
    return ref[part * size:(part + count) * size]


def pack_columns(parts):
    total, offset, out = sum(p.shape[0] for p in parts), 0, 0.0
    for p in parts:
        out = out + lax.pad(p.astype(F32), jnp.float32(0), [(offset, total - offset - p.shape[0], 0)])
        offset += p.shape[0]
    return out[:, None]


def dot_nn(a, b):
    return lax.dot_general(a, b, (((1,), (0,)), ((), ())), preferred_element_type=F32)


def dot_nt(a, b):
    return lax.dot_general(a, b, (((1,), (1,)), ((), ())), preferred_element_type=F32)


I_STRIDE = 24
S_GROUP = 32


def msa_kernel(m_ref, norm_ref, w_ref, bias_ref, *refs):
    y_ref, t_ref = refs[-2:]
    layers = t_ref.shape[0]
    a_refs, b_refs = refs[:layers], refs[layers:2 * layers]
    s_blk, n_i, _ = m_ref.shape
    n_c = b_refs[0].shape[0]
    group = S_GROUP
    gains = [norm_ref[l].astype(F32) for l in range(layers)]

    def rows(g, carry):
        base = pl.multiple_of(g * group, group)
        x = m_ref[pl.ds(base, group)].astype(F32).reshape(group * n_i, -1)
        mean_val = jnp.mean(x, axis=-1, keepdims=True)
        centered = x - mean_val
        var_val = jnp.mean(centered * centered, axis=-1, keepdims=True)
        scaled = centered * lax.rsqrt(var_val + LN_EPS)
        normed = jnp.concatenate([(scaled * gains[l][0:1] + gains[l][1:2]).astype(BF16) for l in range(layers)], axis=1)
        proj = dot_nn(normed, w_ref[...]) + bias_ref[...]
        for s in range(group):
            y_ref[pl.ds(pl.multiple_of((base + s) * I_STRIDE, 8), n_i), :] = proj[s * n_i:(s + 1) * n_i]
        return carry
    lax.fori_loop(0, s_blk // group, rows, 0, unroll=4)

    def columns(i, carry):
        flip = y_ref[pl.ds(i, s_blk, stride=I_STRIDE), :].T
        for l in range(layers):
            top = 2 * l * n_c
            a_refs[l][pl.ds(pl.multiple_of(i * n_c, n_c), n_c), :] = flip[top:top + n_c].astype(BF16)
            t_ref[l, pl.ds(i, n_c, stride=I_STRIDE), :] = flip[top + n_c:top + 2 * n_c]
        return carry
    lax.fori_loop(0, n_i, columns, 0, unroll=8)
    for l in range(layers):
        for d in range(n_c):
            b_refs[l][d] = t_ref[l, d * I_STRIDE:d * I_STRIDE + n_i, :].astype(BF16)


def msa_project(msa_act, norm_w, w_bd, bias):
    seqs, n_i, n_m = msa_act.shape
    layers = norm_w.shape[0]
    n_c = w_bd.shape[1] // (2 * layers)
    s_blk = LANES
    return pl.pallas_call(
        msa_kernel, grid=(seqs // s_blk,),
        in_specs=[
            pl.BlockSpec((s_blk, n_i, n_m), lambda s: (s, 0, 0)),
            pl.BlockSpec(norm_w.shape, lambda s: (0, 0, 0)),
            pl.BlockSpec(w_bd.shape, lambda s: (0, 0)),
            pl.BlockSpec(bias.shape, lambda s: (0, 0)),
        ],
        out_specs=(pl.BlockSpec((n_i * n_c, s_blk), lambda s: (0, s)),) * layers
        + (pl.BlockSpec((n_c, n_i, s_blk), lambda s: (0, 0, s)),) * layers,
        out_shape=(jax.ShapeDtypeStruct((n_i * n_c, seqs), BF16),) * layers
        + (jax.ShapeDtypeStruct((n_c, n_i, seqs), BF16),) * layers,
        scratch_shapes=[pltpu.VMEM((s_blk * I_STRIDE, w_bd.shape[1]), F32),
                        pltpu.VMEM((layers, n_c * I_STRIDE, s_blk), F32)],
        compiler_params=pltpu.CompilerParams(dimension_semantics=('arbitrary',)),
        cost_estimate=pl.CostEstimate(flops=2 * seqs * n_i * n_m * 2 * n_c * layers,
                                      bytes_accessed=2 * seqs * n_i * (n_m + 2 * n_c * layers), transcendentals=0),
        name='msa_project',
    )(msa_act, norm_w, w_bd, bias)


def opm_kernel(inv_s, first, last, a_ref, b_ref, w_ref, bias_ref, *rest):
    acc_ref, out_ref, q_ref = (None,) * first + rest
    part = pl.program_id(1)
    dev, d_blk, j_loc, seqs = b_ref.shape
    n_i, _, j_blk = q_ref.shape
    n_c = a_ref.shape[0] // n_i
    for d in range(d_blk):
        rhs = b_ref[:, d, :, :].reshape(dev * j_loc, seqs)
        prod = (dot_nt(a_ref[...], rhs) * inv_s).astype(BF16)
        base = pl.multiple_of((part * d_blk + d) * n_c, n_c)
        q_ref[:, pl.ds(base, n_c), :] = prod.reshape(n_i, n_c, j_blk)

    @pl.when(part == pl.num_programs(1) - 1)
    def _():
        def body(i, carry):
            upd = dot_nn(w_ref[...], q_ref[i])
            if not first:
                upd = acc_ref[i] + upd
            out_ref[i] = (upd + col(bias_ref, OPM_BIAS)).astype(BF16) if last else upd
            return carry
        lax.fori_loop(0, n_i, body, 0, unroll=4)


def opm_update(a_t, b_all, w_t, bias, acc=None, last=True):
    n_dev, n_d, j_loc, seqs = b_all.shape
    rows_c = a_t.shape[0]
    n_z = w_t.shape[0]
    n_c = w_t.shape[1] // n_d
    n_i = rows_c // n_c
    cols = n_dev * j_loc
    j_blk = 2 * LANES
    dev_blk = j_blk // j_loc
    d_blk = math.gcd(n_d, 8)
    grid = (cols // j_blk, n_d // d_blk)
    row_spec = pl.BlockSpec((n_i, n_z, j_blk), lambda j, d: (0, 0, j))
    first = acc is None
    return pl.pallas_call(
        functools.partial(opm_kernel, 1.0 / seqs, first, last),
        grid=grid,
        in_specs=[
            pl.BlockSpec((rows_c, seqs), lambda j, d: (0, 0)),
            pl.BlockSpec((dev_blk, d_blk, j_loc, seqs), lambda j, d: (j, d, 0, 0)),
            pl.BlockSpec(w_t.shape, lambda j, d: (0, 0)),
            pl.BlockSpec(bias.shape, lambda j, d: (0, 0)),
        ] + ([] if first else [row_spec]),
        out_specs=row_spec,
        out_shape=jax.ShapeDtypeStruct((n_i, n_z, cols), BF16 if last else F32),
        scratch_shapes=[pltpu.VMEM((n_i, n_d * n_c, j_blk), BF16)],
        compiler_params=pltpu.CompilerParams(dimension_semantics=('arbitrary', 'arbitrary')),
        cost_estimate=pl.CostEstimate(
            flops=2 * rows_c * seqs * cols * n_d + 2 * n_i * cols * n_d * n_c * n_z,
            bytes_accessed=2 * (n_dev * n_d * j_loc * seqs + n_i * n_z * cols), transcendentals=0),
        name='opm_update',
    )(a_t, b_all, w_t, bias, *(() if first else (acc,)))


MESH_ID = pl.DeviceIdType.MESH
AG_UNITS = 4


class RingGather:
    def __init__(self, n, axis, src_ref, out_ref, r_sem, p_sem, s_sem, l_sem):
        self.n, self.side, self.axis = n, math.isqrt(n // 2), axis
        self.src, self.out = src_ref, out_ref
        self.r_sem, self.p_sem, self.s_sem, self.l_sem = r_sem, p_sem, s_sem, l_sem
        me = lax.axis_index(axis)
        self.me, self.core = me, me % 2
        self.x, self.y = (me // 2) % self.side, me // (2 * self.side)
        self.size = src_ref.shape[0] // AG_UNITS

    def at(self, u, k1, k2, other=False):
        kx, ky = (k1, k2) if u < AG_UNITS // 2 else (k2, k1)
        core = 1 - self.core if other else self.core
        return (((self.y + ky) % self.side) * self.side + (self.x + kx) % self.side) * 2 + core

    def neighbours(self):
        last = self.side - 1
        return [self.at(0, 1, 0), self.at(0, last, 0), self.at(0, 0, 1), self.at(0, 0, last), self.at(0, 0, 0, True)]

    def barrier(self):
        sem = pltpu.get_barrier_semaphore()
        peers = self.neighbours()
        for p in peers:
            pl.semaphore_signal(sem, inc=1, device_id={self.axis: p}, device_id_type=MESH_ID)
        pl.semaphore_wait(sem, len(peers))

    def copy(self, u, k1, k2, way):
        rows = pl.ds(u * self.size, self.size)
        owner = self.at(u, k1, k2)
        src = self.src.at[rows] if (k1, k2) == (0, 0) else self.out.at[owner, rows]
        step = (1, self.side - 1)[way % 2]
        if way < 2:
            dest, rk, sems = self.at(u, step, 0), ((k1 - step) % self.side, k2), self.r_sem
        elif way < 4:
            dest, rk, sems = self.at(u, 0, step), (k1, (k2 - step) % self.side), self.r_sem
        else:
            dest, rk, sems = self.at(u, 0, 0, True), (k1, k2), self.p_sem
        return pltpu.make_async_remote_copy(src, self.out.at[owner, rows], self.s_sem.at[u, k1, k2, way], sems.at[u, rk[0], rk[1]],
                                            device_id={self.axis: dest}, device_id_type=MESH_ID)

    def ways(self, u, k1, k2):
        last = self.side - 1
        plus = u % 2 == 0
        out = []
        if k2 == 0:
            if k1 == 0:
                out += [0, 1]
            elif k1 == last and plus:
                out.append(0)
            elif k1 == 1 and not plus:
                out.append(1)
            out += [2, 3]
        elif k2 == last and plus:
            out.append(2)
        elif k2 == 1 and not plus:
            out.append(3)
        return out + [4]

    def arrived(self, u, k1, k2, sems, other=False):
        rows = pl.ds(u * self.size, self.size)
        dst = self.out.at[self.at(u, k1, k2, other), rows]
        pltpu.make_async_remote_copy(dst, dst, self.s_sem.at[u, k1, k2, 4], sems.at[u, k1, k2],
                                     device_id={self.axis: self.at(0, 0, 0, True)}, device_id_type=MESH_ID).wait_recv()

    def steps(self):
        last = self.side - 1
        units = range(AG_UNITS)
        own = pltpu.make_async_copy(self.src, self.out.at[self.me], self.l_sem)

        def begin():
            own.start()
            for pair in ((0, 1), (2, 3), (4,)):
                for u in units:
                    for way in pair:
                        self.copy(u, 0, 0, way).start()

        def relay(k1, k2):
            for u in units:
                self.arrived(u, k1, k2, self.r_sem)
                for way in self.ways(u, k1, k2):
                    self.copy(u, k1, k2, way).start()

        def finish():
            for k1 in range(self.side):
                for k2 in range(self.side):
                    for u in units:
                        self.arrived(u, k1, k2, self.p_sem, True)
            for k1 in range(self.side):
                for k2 in range(self.side):
                    for u in units:
                        for way in self.ways(u, k1, k2):
                            self.copy(u, k1, k2, way).wait_send()
            own.wait()
        order = [(last, 0), (1, 0), (0, last), (0, 1), (2, 0)]
        order += [(k1, k2) for k1 in (last, 1, 2) for k2 in (last, 1)]
        order += [(k1, 2) for k1 in (0, last, 1, 2)]
        return [begin] + [functools.partial(relay, *o) for o in order] + [finish]


def gather_kernel(n, axis, src_ref, out_ref, *sems):
    ring = RingGather(n, axis, src_ref, out_ref, *sems)
    ring.barrier()
    for step in ring.steps():
        step()


def gather_scratch(side):
    dma = pltpu.SemaphoreType.DMA
    return [dma((AG_UNITS, side, side)), dma((AG_UNITS, side, side)), dma((AG_UNITS, side, side, 5)), dma]


def ring_gather(block, n, axis, cid):
    side = math.isqrt(n // 2)
    assert 2 * side * side == n and side == 4
    return pl.pallas_call(
        functools.partial(gather_kernel, n, axis),
        out_shape=jax.ShapeDtypeStruct((n,) + block.shape, block.dtype),
        in_specs=[pl.BlockSpec(memory_space=pl.ANY)], out_specs=pl.BlockSpec(memory_space=pl.ANY),
        scratch_shapes=gather_scratch(side),
        compiler_params=pltpu.CompilerParams(collective_id=cid, has_side_effects=True),
        name='ring_gather',
    )(block)


def gather_opm_kernel(n, axis, inv_s, src_ref, a_ref, b_ref, w_ref, c_ref, z_ref, mask_ref, w_ab_ref, out_ref, z_out, ab_ref,
                      buf, q_ref, upd_ref, s_a, s_b, b_sem, *sems):
    ring = RingGather(n, axis, src_ref, out_ref, *sems)
    _, dev_blk, d_blk, j_loc, seqs = buf.shape
    n_i, _, j_blk = q_ref.shape
    n_c = a_ref.shape[0] // n_i
    parts = b_ref.shape[1] // d_blk
    total = (b_ref.shape[0] // dev_blk) * parts

    def load(k):
        j, part = k // parts, k % parts
        return pltpu.make_async_copy(b_ref.at[pl.ds(j * dev_blk, dev_blk), pl.ds(part * d_blk, d_blk)], buf.at[k % 2], b_sem.at[k % 2])

    def outer(k):
        if k + 1 < total:
            load(k + 1).start()
        load(k).wait()

        def body(d, carry):
            rhs = buf[k % 2, :, d].reshape(dev_blk * j_loc, seqs)
            prod = (dot_nt(a_ref[...], rhs) * inv_s).astype(BF16)
            base = pl.multiple_of(((k % parts) * d_blk + d) * n_c, n_c)
            q_ref[:, pl.ds(base, n_c), :] = prod.reshape(n_i, n_c, j_blk)
            return carry
        lax.fori_loop(0, d_blk, body, 0, unroll=2)

    def contract(j, low, high):
        def body(i, carry):
            upd = dot_nn(w_ref[...], q_ref[i]) + col(c_ref, OPM_BIAS)
            upd_ref[i, :, j * j_blk:(j + 1) * j_blk] = upd.astype(BF16)
            return carry
        lax.fori_loop(low, high, body, 0, unroll=4)
    pieces = []
    for k in range(total):
        pieces.append(functools.partial(outer, k))
        if k % parts == parts - 1:
            for half in range(2):
                pieces.append(functools.partial(contract, k // parts, half * n_i // 2, (half + 1) * n_i // 2))

    def project(j, low, high):
        lanes = slice(j * j_blk, (j + 1) * j_blk)

        def body(i, carry):
            z_old = z_ref[i, lanes, :].astype(F32).T
            z_new = (z_old + upd_ref[i, :, lanes].astype(F32)).astype(BF16)
            z_out[i, :, lanes] = z_new
            project_row(i, z_new.astype(F32), mask_ref[pl.ds(i, 1), lanes].astype(F32), w_ab_ref, c_ref, (s_a, s_b),
                        j * j_blk // LANES)
            return carry
        lax.fori_loop(low, high, body, 0, unroll=2)
    for j in range(total // parts):
        for quarter in range(4):
            pieces.append(functools.partial(project, j, quarter * n_i // 4, (quarter + 1) * n_i // 4))
    n_dest = ab_ref.shape[0]
    for half in range(2):
        pieces.append(functools.partial(emit_ab, ab_ref, (s_a, s_b), half * n_dest // 2, (half + 1) * n_dest // 2))
    load(0).start()
    ring.barrier()
    steps = ring.steps()
    done = 0
    for k, step in enumerate(steps[:-1]):
        step()
        while done * (len(steps) - 1) < (k + 1) * len(pieces):
            pieces[done]()
            done += 1
    steps[-1]()


def gather_with_opm(block, n, axis, cid, a_t, b_all, w_t, cols_l, pair_act, pair_mask, w_ab):
    n_dev, n_d, j_loc, seqs = b_all.shape
    n_z = w_t.shape[0]
    n_c = w_t.shape[1] // n_d
    n_i = a_t.shape[0] // n_c
    cols = n_dev * j_loc
    j_blk = 2 * LANES
    d_blk = math.gcd(n_d, 8)
    side = math.isqrt(n // 2)
    assert 2 * side * side == n and side == 4
    ab_scr = pltpu.VMEM((cols // LANES, n_z * I_STRIDE, LANES), F32)
    any_spec = pl.BlockSpec(memory_space=pl.ANY)
    vmem_spec = pl.BlockSpec(memory_space=pltpu.VMEM)
    return pl.pallas_call(
        functools.partial(gather_opm_kernel, n, axis, 1.0 / seqs),
        out_shape=(jax.ShapeDtypeStruct((n,) + block.shape, block.dtype), jax.ShapeDtypeStruct((n_i, n_z, cols), BF16),
                   jax.ShapeDtypeStruct((n, 2, n_z // n, n_i, cols), BF16)),
        in_specs=[any_spec, vmem_spec, any_spec] + [vmem_spec] * 5, out_specs=(any_spec, vmem_spec, vmem_spec),
        scratch_shapes=[pltpu.VMEM((2, j_blk // j_loc, d_blk, j_loc, seqs), BF16), pltpu.VMEM((n_i, n_d * n_c, j_blk), BF16),
                        pltpu.VMEM((n_i, n_z, cols), BF16), ab_scr, ab_scr, pltpu.SemaphoreType.DMA((2,))] + gather_scratch(side),
        compiler_params=pltpu.CompilerParams(collective_id=cid, has_side_effects=True),
        cost_estimate=pl.CostEstimate(flops=2 * a_t.shape[0] * seqs * cols * n_d * 4, bytes_accessed=2 * b_all.size, transcendentals=0),
        name='ring_gather_opm',
    )(block, a_t, b_all, w_t, cols_l, pair_act, pair_mask, w_ab)


def norm_columns(x_f32, gain, offset):
    mean_val = jnp.mean(x_f32, axis=0, keepdims=True)
    centered = x_f32 - mean_val
    var_val = jnp.mean(centered * centered, axis=0, keepdims=True)
    return (centered * lax.rsqrt(var_val + LN_EPS) * gain + offset).astype(BF16)


def sigmoid(x):
    return 0.5 * jnp.tanh(0.5 * x) + 0.5


def project_row(i, z_f32, mask_row, w_ref, c_ref, s_refs, tile0=0):
    zn = norm_columns(z_f32, col(c_ref, NORM_IN), col(c_ref, NORM_IN + 1))
    n_z, lanes = z_f32.shape
    n_ch = w_ref.shape[0] // 4
    proj = dot_nn(w_ref[...], zn) + col(c_ref, PROJ_BIAS, 4)
    for q in range(2):
        lin = proj[2 * q * n_ch:(2 * q + 1) * n_ch]
        sig = sigmoid(proj[(2 * q + 1) * n_ch:(2 * q + 2) * n_ch])
        val = mask_row * sig * lin
        for t in range(lanes // LANES):
            s_refs[q][tile0 + t, pl.ds(i, n_ch, stride=I_STRIDE), :] = val[:, t * LANES:(t + 1) * LANES]


def gate_kernel(z_ref, w_ref, c_ref, gate_ref):
    def body(i, carry):
        zn = norm_columns(z_ref[i].astype(F32), col(c_ref, NORM_IN), col(c_ref, NORM_IN + 1))
        gate_ref[i] = sigmoid(dot_nn(w_ref[...], zn) + col(c_ref, GATE_BIAS))
        return carry
    lax.fori_loop(0, z_ref.shape[0], body, 0, unroll=4)


def gate_call(z_t, w_gate, cols_l):
    n_i, n_z, cols = z_t.shape
    row_spec = pl.BlockSpec((n_i, n_z, J_BLK), lambda j: (0, 0, j))
    return pl.pallas_call(
        gate_kernel, grid=(cols // J_BLK,),
        in_specs=[row_spec, pl.BlockSpec(w_gate.shape, lambda j: (0, 0)), pl.BlockSpec(cols_l.shape, lambda j: (0, 0))],
        out_specs=row_spec, out_shape=jax.ShapeDtypeStruct(z_t.shape, F32),
        compiler_params=pltpu.CompilerParams(dimension_semantics=('arbitrary',)),
        cost_estimate=pl.CostEstimate(flops=12 * n_i * cols * n_z * n_z, bytes_accessed=6 * n_i * cols * n_z,
                                      transcendentals=n_i * cols * n_z),
        name='tri_gate',
    )(z_t, w_gate, cols_l)


def emit_ab(ab_ref, s_refs, low=0, high=None):
    n_dev, _, n_cl, n_i, lanes = ab_ref.shape
    high = n_dev if high is None else high

    def body(dev, carry):
        for q in range(2):
            for c in range(n_cl):
                base = pl.multiple_of((dev * n_cl + c) * I_STRIDE, 8)
                for t in range(lanes // LANES):
                    ab_ref[dev, q, c, :, t * LANES:(t + 1) * LANES] = s_refs[q][t, pl.ds(base, n_i), :].astype(BF16)
        return carry
    lax.fori_loop(low, high, body, 0, unroll=2)


def finish_stats(o_ref, s_o, r_ref):
    n_c, n_i, lanes = o_ref.shape
    total = lax.fori_loop(0, n_c, lambda c, acc: acc + o_ref[c], jnp.zeros((n_i, lanes), F32), unroll=16)
    mean_val = total / n_c

    def body(c, acc):
        base = pl.multiple_of(c * I_STRIDE, 8)
        centered = o_ref[c] - mean_val
        for t in range(lanes // LANES):
            s_o[t, pl.ds(base, n_i), :] = centered[:, t * LANES:(t + 1) * LANES]
        return acc + centered * centered
    square = lax.fori_loop(0, n_c, body, jnp.zeros((n_i, lanes), F32), unroll=16)
    r_ref[...] = lax.rsqrt(square / n_c + LN_EPS)


def finish_row(i, z_ref, gate_ref, wo_ref, c_ref, s_o, r_ref):
    tiles, rows, _ = s_o.shape
    n_c = rows // I_STRIDE
    centered = jnp.concatenate([s_o[t, pl.ds(i, n_c, stride=I_STRIDE), :] for t in range(tiles)], axis=1)
    norm = (centered * r_ref[pl.ds(i, 1), :] * col(c_ref, NORM_OUT) + col(c_ref, NORM_OUT + 1)).astype(BF16)
    upd = (dot_nn(wo_ref[...], norm) + col(c_ref, OUT_BIAS)).astype(BF16)
    return (z_ref[i].astype(F32) + gate_ref[i] * upd.astype(F32)).astype(BF16)


def middle_kernel(o_ref, zin_ref, gin_ref, wo_ref, cp_ref, u_ref, mask_ref, w_ref, c_ref,
                  z_out, ab_ref, s_a, s_b, s_o, r_ref):
    n_i = zin_ref.shape[0]
    finish_stats(o_ref, s_o, r_ref)

    def body(i, carry):
        z_mid = finish_row(i, zin_ref, gin_ref, wo_ref, cp_ref, s_o, r_ref)
        z_new = (z_mid.astype(F32) + u_ref[i].astype(F32)).astype(BF16)
        z_out[i] = z_new
        project_row(i, z_new.astype(F32), mask_ref[pl.ds(i, 1), :].astype(F32), w_ref, c_ref, (s_a, s_b))
        return carry
    lax.fori_loop(0, n_i, body, 0, unroll=ROW_UNROLL)
    emit_ab(ab_ref, (s_a, s_b))


def end_kernel(o_ref, zin_ref, gin_ref, wo_ref, c_ref, z_out, s_o, r_ref):
    n_i = zin_ref.shape[0]
    finish_stats(o_ref, s_o, r_ref)

    def body(i, carry):
        z_new = finish_row(i, zin_ref, gin_ref, wo_ref, c_ref, s_o, r_ref)
        z_out[i] = z_new.astype(F32).T.astype(BF16)
        return carry
    lax.fori_loop(0, n_i, body, 0, unroll=ROW_UNROLL)


J_BLK = 256


def tri_call(kind, n_dev, args):
    kernels = {'middle': middle_kernel, 'end': end_kernel}
    n_i, n_z, cols = args[1].shape
    n_ch = n_z

    def blk(arr, which):
        shape = arr.shape
        if which == 'j':
            return pl.BlockSpec(shape[:-1] + (J_BLK,), lambda j: (0,) * (len(shape) - 1) + (j,))
        return pl.BlockSpec(shape, lambda j: (0,) * len(shape))

    tiles = J_BLK // LANES
    fin = ['j', 'j', 'j', 'w', 'w']
    kinds = {'middle': fin + ['j', 'j', 'w', 'w'], 'end': fin}[kind]
    scr = pltpu.VMEM((tiles, n_ch * I_STRIDE, LANES), F32)
    stat = pltpu.VMEM((n_i, J_BLK), F32)
    if kind == 'end':
        out_shape = jax.ShapeDtypeStruct((n_i, cols, n_z), BF16)
        out_specs = pl.BlockSpec((n_i, J_BLK, n_z), lambda j: (0, j, 0))
        scratch = [scr, stat]
    else:
        out_shape = (jax.ShapeDtypeStruct((n_i, n_z, cols), BF16),
                     jax.ShapeDtypeStruct((n_dev, 2, n_ch // n_dev, n_i, cols), BF16))
        out_specs = tuple(blk(s, 'j') for s in out_shape)
        scratch = [scr, scr] + ([scr, stat] if kind == 'middle' else [])
    return pl.pallas_call(
        kernels[kind], grid=(cols // J_BLK,),
        in_specs=[blk(a, k) for a, k in zip(args, kinds)],
        out_specs=out_specs, out_shape=out_shape, scratch_shapes=scratch,
        compiler_params=pltpu.CompilerParams(dimension_semantics=('arbitrary',)),
        cost_estimate=pl.CostEstimate(flops=12 * n_i * cols * n_z * n_z, bytes_accessed=16 * n_i * cols * n_z,
                                      transcendentals=3 * n_i * cols * n_z),
        name='tri_' + kind,
    )(*args)


def product_kernel(ab_ref, o_ref):
    n_dev, _, _, n_i, cols = ab_ref.shape
    left = ab_ref[:, 0, 0].reshape(n_dev * n_i, cols)
    right = ab_ref[:, 1, 0].reshape(n_dev * n_i, cols)
    half = cols // 2
    for h in range(2):
        o_ref[:, 0, :, h * half:(h + 1) * half] = dot_nt(left, right[h * half:(h + 1) * half]).reshape(n_dev, n_i, half)


def tri_product(ab):
    n_dev, _, n_cl, n_i, cols = ab.shape
    rows = n_dev * n_i
    return pl.pallas_call(
        product_kernel, grid=(n_cl,),
        in_specs=[pl.BlockSpec((n_dev, 2, 1, n_i, cols), lambda c: (0, 0, c, 0, 0))],
        out_specs=pl.BlockSpec((n_dev, 1, n_i, cols), lambda c: (0, c, 0, 0)),
        out_shape=jax.ShapeDtypeStruct((n_dev, n_cl, n_i, cols), F32),
        compiler_params=pltpu.CompilerParams(dimension_semantics=('arbitrary',)),
        cost_estimate=pl.CostEstimate(flops=2 * n_cl * rows * rows * cols, bytes_accessed=8 * n_cl * rows * cols,
                                      transcendentals=0),
        name='tri_product',
    )(ab)


def solution(mesh):
    pair_spec = P(('batch', 'dap'), None, None)
    mask_spec = P(('batch', 'dap'), None)
    msa_spec = P(None, ('batch', 'dap'), None)
    n_dev = mesh.shape['dap']

    def device_fn(pair_act, pair_mask, msa_act, opm_norm, opm_w_in, opm_b_in, opm_w_out, opm_b_out, tri_norm_in, tri_w_ab, tri_b_ab, tri_w_gate, tri_b_gate, tri_norm_out, tri_w_out, tri_b_out):
        layers = opm_norm.shape[0]
        assert layers == 2
        n_i, cols, n_z = pair_act.shape
        n_c = opm_w_in.shape[-1]
        n_m = msa_act.shape[-1]
        same = jnp.arange(layers)[:, None] == jnp.arange(layers)[None, :]
        w_bd = jnp.where(same[:, None, :, None], opm_w_in.reshape(layers, n_m, 1, 2 * n_c), 0)
        sides = msa_project(msa_act, opm_norm, w_bd.reshape(layers * n_m, layers * 2 * n_c).astype(BF16),
                            opm_b_in.astype(F32).reshape(1, -1))
        left, right = sides[:layers], sides[layers:]
        opm_w = [opm_w_out[l].reshape(n_c, n_c, n_z).transpose(2, 1, 0).reshape(n_z, n_c * n_c) for l in range(layers)]
        w_abs = [tri_w_ab[l].transpose(1, 2, 0).reshape(-1, n_z) for l in range(layers)]
        params = [pack_columns([p[l].reshape(-1) for p in (opm_b_out, tri_norm_in, tri_b_ab, tri_b_gate, tri_norm_out, tri_b_out)])
                  for l in range(layers)]
        gathered = ring_gather(right[0], n_dev, 'dap', 0)
        gathered, z_t, ab = gather_with_opm(right[1], n_dev, 'dap', 1, left[0], gathered, opm_w[0], params[0], pair_act, pair_mask,
                                            w_abs[0])
        update = opm_update(left[1], gathered, opm_w[1], params[1])
        fin = None
        for l in range(layers):
            if l:
                z_t, ab = tri_call('middle', n_dev, fin + (update, pair_mask, w_abs[l], params[l]))
            ab = lax.all_to_all(ab.reshape(n_dev, -1, cols), 'dap', 0, 0, tiled=True).reshape(ab.shape)
            prod, z_g = lax.optimization_barrier((tri_product(ab), z_t))
            gate = gate_call(z_g, tri_w_gate[l].T, params[l])
            prod = lax.all_to_all(prod, 'dap', 0, 0, tiled=True)
            fin = (prod.reshape(-1, n_i, cols), z_t, gate, tri_w_out[l].T, params[l])
        return tri_call('end', n_dev, fin)

    return jax.shard_map(device_fn, mesh=mesh, in_specs=(pair_spec, mask_spec, msa_spec) + (P(),) * 13, out_specs=pair_spec, check_vma=False)
```
